256 devices in a mesh: groups: 4 (over y, x), gx: 32 (over z), gy: 2 (over core).
Axes of the slice: x: 2, y: 2, z: 32, core: 2. Of those that a mesh axis runs over, the one named last changes fastest.
The devices are a block of a 4x8x32 slice.
Arguments:
- initial_voltage: float32 [2048, 128, 256], P(('groups', 'gx'), 'gy'), parts along dimension 0, may hold values from -0.1 to 1.1
- conductivity: float32 [2048, 128, 256], P(('groups', 'gx'), 'gy'), parts along dimension 0, may hold values from 0.3 to 1.2
- tissue_mask: int32 [2048, 128, 256], P(('groups', 'gx'), 'gy'), parts along dimension 0, may hold values 0 or 1
- target_step: int32 [2048, 128, 256], P(('groups', 'gx'), 'gy'), parts along dimension 0, may hold values from 0 to 8
- initial_purkinje: float32 [131072, 128], P(('groups', 'gx', 'gy')), parts along dimension 0, may hold values from -0.1 to 1.1
- purkinje_conductivity: float32 [131072], P(('groups', 'gx', 'gy')), parts along dimension 0, may hold values from 0.5 to 4
- segment_parent: int32 [131072], P(('groups', 'gx', 'gy')), parts along dimension 0, may hold values from -1 to 32766, as said below
- purkinje_target: int32 [131072, 128], P(('groups', 'gx', 'gy')), parts along dimension 0, may hold values from 0 to 8
- junction_voxel: int32 [131072], P(('groups', 'gx', 'gy')), parts along dimension 0, may hold values from 0 to 16777215, as said below
- junction_node: int32 [131072], P(('groups', 'gx', 'gy')), parts along dimension 0, may hold values from 0 to 4194303, as said below
Outputs:
- final_voltage: float32 [2048, 128, 256], P(('groups', 'gx'), 'gy'), parts along dimension 0
- final_purkinje: float32 [131072, 128], P(('groups', 'gx', 'gy')), parts along dimension 0
- conductivity_gradient: float32 [2048, 128, 256], P(('groups', 'gx'), 'gy'), parts along dimension 0
- purkinje_gradient: float32 [131072], P(('groups', 'gx', 'gy')), parts along dimension 0
- voltage_adjoint: float32 [2048, 128, 256], P(('groups', 'gx'), 'gy'), parts along dimension 0
- purkinje_adjoint: float32 [131072, 128], P(('groups', 'gx', 'gy')), parts along dimension 0
The draws below stay inside these ranges and needn't reach their ends.
There are 4 independent parts, one for each index of `groups`. The reference program is written for one: setup_inputs(seed, part) draws one part's arguments, and reference() takes and returns one part's arrays. A program takes and returns all parts, laid end to end along the dimension named above; each array names one. Nothing has to cross between parts.
Inputs may be any that keep to these rules, and one draw needn't show every extreme that they name: `junction_voxel`: A flat voxel index (x * 128 + y) * 256 + z. Among the 512 entries of one device's block, at most 16 lie in the voxel block of one tissue device, and some tissue device holds exactly 16 junctions of every device's block. `junction_node`: A flat node index s * 128 + i; the segment s of entry k lies in the same device block as entry k (block k // 512). `segment_parent`: -1 marks a root; otherwise the number of an earlier segment, at most 1024 before it.
All inputs are finite; a program needn't handle non-finite values. No bound on the sum of `tissue_mask` on one device may be relied on, other than what follows from the above.
Results may differ from the reference program's by a relative error of at most 0.0001.
Values sent between devices are 32-bit elements; how exact they have to be, the bound alone decides.
No kernel may reach another device: no remote copies, remote signals or barrier semaphores. Data moves between devices by JAX's collectives and lax.ppermute only.
A program may use at most 128 MiB of HBM per device.

```python
import math
import jax
import jax.numpy as jnp
from jax import lax

CX = 16
CY = 64
CZ = 256
SPD = 512
SEG = 128
JPD = 512
NX = 512
NY = 128
NSEG = 32768
CAP = 16
N_GX = 32
N_GY = 2


def junction_plan(key):
    folded = jax.random.fold_in(key, 4242)
    subkeys = jax.random.split(folded, 6)
    devices = N_GX * N_GY
    slot_count = devices * CAP
    ranking = jax.random.permutation(subkeys[0], devices)
    priority = jnp.where(ranking < 2, 3, jnp.where(ranking < 2 + devices // 8, 2, jnp.where(ranking < devices // 2, 1, 0)))
    slot_number = jnp.arange(slot_count, dtype=jnp.int32)
    slot_device = slot_number // CAP
    jitter = jax.random.randint(subkeys[1], (devices, slot_count), 0, 4096)
    scores = (priority[slot_device][None, :] * 4096 + jitter) * slot_count + slot_number[None, :]
    chosen = jnp.sort(lax.top_k(scores, JPD)[1], axis=1)
    target = chosen // CAP
    offset_first = jax.random.randint(subkeys[2], (devices, JPD), 0, CX)
    offset_second = jax.random.randint(subkeys[3], (devices, JPD), 0, CY)
    offset_third = jax.random.randint(subkeys[4], (devices, JPD), 0, CZ)
    coord_first = target // N_GY * CX + offset_first
    coord_second = target % N_GY * CY + offset_second
    voxel_index = (coord_first * NY + coord_second) * CZ + offset_third
    source = jnp.arange(devices, dtype=jnp.int32)[:, None]
    purkinje_node = source * (SPD * SEG) + jax.random.randint(subkeys[5], (devices, JPD), 0, SPD * SEG)
    return (voxel_index.reshape(-1).astype(jnp.int32), purkinje_node.reshape(-1).astype(jnp.int32))


def draw_junction_voxel(key, part):
    return junction_plan(key)[0]


def draw_junction_node(key, part):
    return junction_plan(key)[1]


def draw_segment_parent(key, part):
    folded = jax.random.fold_in(key, 777)
    number = jnp.arange(NSEG, dtype=jnp.int32)
    distance = jax.random.randint(folded, (NSEG,), 1, 2 * SPD + 1)
    earlier = number - distance
    return jnp.where(earlier < 0, -1, earlier).astype(jnp.int32)


def set_ends(array, own_key, smallest, largest):
    shape = array.shape
    spot = [jax.random.randint(jax.random.fold_in(own_key, axis), (), 0, shape[axis]) for axis in range(len(shape))]
    array = array.at[tuple(spot)].set(smallest)
    longest = shape.index(max(shape))
    spot[longest] = (spot[longest] + 1) % shape[longest]
    return array.at[tuple(spot)].set(largest)


def block_scale(own_key, extent, shards, least, top_value):
    loudness = 1.0
    for dim, shards_of in shards:
        steps = jax.random.uniform(jax.random.fold_in(jax.random.fold_in(own_key, 6), dim), (shards_of,), jnp.float32, least / len(shards), top_value / len(shards))
        loudness = loudness * jnp.repeat(jnp.exp(steps), extent[dim] // shards_of).reshape((-1,) + (1,) * (len(extent) - 1 - dim))
    return loudness


def setup_inputs(seed: int = 0, part: int = 0) -> dict:
    splits = jax.random.split(jax.random.key(seed), 11)
    part_keys = jax.random.split(jax.random.fold_in(splits[10], part), 11)
    initial_voltage = jnp.clip(-0.1 + 1.2 * jax.random.uniform(part_keys[0], (NX, NY, CZ), jnp.float32) ** block_scale(part_keys[0], (NX, NY, CZ), ((0, 32), (1, 2)), -0.2, 0.2), -0.1, 1.1)
    conductivity = jnp.clip(jnp.exp(math.log(1.2) - 1.3862944 * jax.random.uniform(part_keys[1], (NX, NY, CZ), jnp.float32) ** block_scale(part_keys[1], (NX, NY, CZ), ((0, 32), (1, 2)), -0.2, 0.2)), 0.3, 1.2)
    tissue_mask = set_ends((jax.random.randint(part_keys[2], (NX, NY, CZ), 0, 8) < 7).astype(jnp.int32), jax.random.fold_in(part_keys[2], 1), 0, 1)
    target_step = set_ends(jax.random.randint(part_keys[3], (NX, NY, CZ), 0, 9), jax.random.fold_in(part_keys[3], 1), 0, 8).astype(jnp.int32)
    initial_purkinje = jnp.clip(-0.1 + 1.2 * jax.random.uniform(part_keys[4], (NSEG, SEG), jnp.float32) ** block_scale(part_keys[4], (NSEG, SEG), ((0, 64),), -0.2, 0.2), -0.1, 1.1)
    purkinje_conductivity = jnp.clip(jnp.exp(math.log(4.0) - 2.0794415 * jax.random.uniform(part_keys[5], (NSEG,), jnp.float32) ** block_scale(part_keys[5], (NSEG,), ((0, 64),), -0.2, 0.2)), 0.5, 4.0)
    segment_parent = draw_segment_parent(jax.random.fold_in(jax.random.fold_in(splits[10], part), 71), part)
    purkinje_target = set_ends(jax.random.randint(part_keys[7], (NSEG, SEG), 0, 9), jax.random.fold_in(part_keys[7], 1), 0, 8).astype(jnp.int32)
    junction_voxel = draw_junction_voxel(jax.random.fold_in(jax.random.fold_in(splits[10], part), 71), part)
    junction_node = draw_junction_node(jax.random.fold_in(jax.random.fold_in(splits[10], part), 71), part)
    return {"initial_voltage": initial_voltage, "conductivity": conductivity, "tissue_mask": tissue_mask, "target_step": target_step, "initial_purkinje": initial_purkinje, "purkinje_conductivity": purkinje_conductivity, "segment_parent": segment_parent, "purkinje_target": purkinje_target, "junction_voxel": junction_voxel, "junction_node": junction_node}


time_step = 0.05
gap_conductance = 4.0
ion_rate = 8.0
threshold = 0.15
loss_weight = 10.0
target_span = 8.0


def ionic(values):
    return ion_rate * values * (values - threshold) * (1.0 - values)


def slope(values):
    return ion_rate * (-3.0 * values * values + 2.0 * (1.0 + threshold) * values - threshold)


def neighbours(padded):
    return [padded[2:, 1:-1, 1:-1], padded[:-2, 1:-1, 1:-1], padded[1:-1, 2:, 1:-1],
            padded[1:-1, :-2, 1:-1], padded[1:-1, 1:-1, 2:], padded[1:-1, 1:-1, :-2]]


def cable(values, gains, safe_parent, has_parent):
    difference = values[:, 1:] - values[:, :-1]
    edge_flux = gains[:, None] * difference
    result = jnp.pad(edge_flux, ((0, 0), (0, 1))) - jnp.pad(edge_flux, ((0, 0), (1, 0)))
    parent_tail = values[safe_parent, -1]
    head_flux = jnp.where(has_parent, gains * (parent_tail - values[:, 0]), 0.0)
    tail_inflow = jnp.zeros(values.shape[0], values.dtype).at[safe_parent].add(-head_flux)
    result = result.at[:, 0].add(head_flux).at[:, -1].add(tail_inflow)
    return result, parent_tail


def junction(tissue_values, cable_values, junction_voxel, junction_node):
    tissue_at = tissue_values.reshape(-1)[junction_voxel]
    cable_at = cable_values.reshape(-1)[junction_node]
    current = gap_conductance * (cable_at - tissue_at)
    into_tissue = jnp.zeros(tissue_values.size, tissue_values.dtype).at[junction_voxel].add(current)
    into_cable = jnp.zeros(cable_values.size, cable_values.dtype).at[junction_node].add(current)
    return into_tissue.reshape(tissue_values.shape), into_cable.reshape(cable_values.shape)


def reference(initial_voltage, conductivity, tissue_mask, target_step, initial_purkinje,
              purkinje_conductivity, segment_parent, purkinje_target, junction_voxel, junction_node):
    mask_float = tissue_mask.astype(jnp.float32)
    sigma_beside = neighbours(jnp.pad(conductivity, 1))
    mask_beside = neighbours(jnp.pad(mask_float, 1))
    conduct = [0.5 * (conductivity + other_sigma) * mask_float * other_mask
               for other_sigma, other_mask in zip(sigma_beside, mask_beside)]
    halves = [0.5 * mask_float * other_mask for other_mask in mask_beside]
    has_parent = segment_parent >= 0
    parent_float = has_parent.astype(jnp.float32)
    safe_parent = jnp.where(has_parent, segment_parent, 0).astype(jnp.int32)

    def tissue_apply(values):
        beside = neighbours(jnp.pad(values, 1))
        total = jnp.zeros_like(values)
        for weight, other in zip(conduct, beside):
            total = total + weight * (other - values)
        return total, beside

    voltage = initial_voltage
    purkinje = initial_purkinje
    history = []
    for repeat in range(2):
        flux_tissue, beside = tissue_apply(voltage)
        flux_cable, parent_tail = cable(purkinje, purkinje_conductivity, safe_parent, has_parent)
        into_tissue, into_cable = junction(voltage, purkinje, junction_voxel, junction_node)
        history.append((voltage, purkinje, beside, parent_tail))
        voltage, purkinje = (voltage + time_step * (flux_tissue + ionic(voltage) + into_tissue),
                             purkinje + time_step * (flux_cable + ionic(purkinje) - into_cable))
    adjoint_voltage = loss_weight * mask_float * (voltage - (1.0 - target_step.astype(jnp.float32) / target_span))
    adjoint_cable = loss_weight * (purkinje - (1.0 - purkinje_target.astype(jnp.float32) / target_span))
    grad_sigma = jnp.zeros_like(voltage)
    grad_cable = jnp.zeros_like(purkinje_conductivity)
    for state in reversed(history):
        old_voltage, old_purkinje, old_beside, old_tail = state
        flux_tissue, adjoint_beside = tissue_apply(adjoint_voltage)
        flux_cable, adjoint_tail = cable(adjoint_cable, purkinje_conductivity, safe_parent, has_parent)
        into_tissue, into_cable = junction(adjoint_voltage, adjoint_cable, junction_voxel, junction_node)
        total = jnp.zeros_like(voltage)
        for half, other_adjoint, other_voltage in zip(halves, adjoint_beside, old_beside):
            total = total + half * (adjoint_voltage - other_adjoint) * (other_voltage - old_voltage)
        grad_sigma = grad_sigma + time_step * total
        inner = jnp.sum((adjoint_cable[:, :-1] - adjoint_cable[:, 1:]) * (old_purkinje[:, 1:] - old_purkinje[:, :-1]), axis=1)
        head = parent_float * (adjoint_cable[:, 0] - adjoint_tail) * (old_tail - old_purkinje[:, 0])
        grad_cable = grad_cable + time_step * (inner + head)
        adjoint_voltage, adjoint_cable = (
            adjoint_voltage + time_step * (flux_tissue + slope(old_voltage) * adjoint_voltage + into_tissue),
            adjoint_cable + time_step * (flux_cable + slope(old_purkinje) * adjoint_cable - into_cable))
    return voltage, purkinje, grad_sigma, grad_cable, adjoint_voltage, adjoint_cable
```

```python
import functools

import jax
import jax.numpy as jnp
from jax import lax
from jax.experimental import pallas as pl
from jax.experimental.pallas import tpu as pltpu
from jax.sharding import PartitionSpec as P

time_step = 0.05
gap_conductance = 4.0
ion_rate = 8.0
threshold = 0.15
loss_weight = 10.0
target_span = 8.0

INTERPRET = False
f32 = jnp.float32
bf16 = jnp.bfloat16
i32 = jnp.int32
FAR = -1.0e7


def sds(shape, dtype=f32):
    return jax.ShapeDtypeStruct(shape, dtype)


def call(kernel, name, outs, scalars, *arrays, flops=2_000_000, limit=24 << 20, scratch=()):
    specs = [pl.BlockSpec(memory_space=pltpu.SMEM)] if scalars is not None else []
    specs += [pl.BlockSpec(memory_space=pltpu.VMEM)] * len(arrays)
    args = ([scalars] if scalars is not None else []) + list(arrays)
    return pl.pallas_call(
        kernel,
        name=name,
        out_shape=outs,
        in_specs=specs,
        out_specs=[pl.BlockSpec(memory_space=pltpu.VMEM)] * len(outs),
        scratch_shapes=list(scratch),
        compiler_params=pltpu.CompilerParams(vmem_limit_bytes=limit),
        cost_estimate=pl.CostEstimate(flops=flops, transcendentals=0, bytes_accessed=4_000_000),
        interpret=INTERPRET,
    )(*args)


def ionic(values):
    return ion_rate * values * (values - threshold) * (1.0 - values)


def slope(values):
    return ion_rate * (-3.0 * values * values + 2.0 * (1.0 + threshold) * values - threshold)


def iota(shape, dim):
    return lax.broadcasted_iota(i32, shape, dim)


def parts(values):
    high = values.astype(bf16)
    rest = values - high.astype(f32)
    middle = rest.astype(bf16)
    low = (rest - middle.astype(f32)).astype(bf16)
    return high, middle, low


def exact_dot(chooser, pieces):
    total = None
    for piece in pieces:
        term = jnp.dot(chooser, piece, preferred_element_type=f32)
        total = term if total is None else total + term
    return total


def one_hot(test):
    return jnp.where(test, 1.0, 0.0).astype(bf16)


def to_row(column):
    count = column.shape[0]
    eye = iota((128, 128), 0) == iota((128, 128), 1)
    rows = []
    for first in range(0, count, 128):
        spread = jnp.broadcast_to(column[first : first + 128], (128, 128))
        rows.append(jnp.sum(jnp.where(eye, spread, 0.0), axis=0, keepdims=True))
    return jnp.concatenate(rows, axis=1)


def to_column(row):
    count = row.shape[1]
    eye = iota((128, 128), 0) == iota((128, 128), 1)
    columns = []
    for first in range(0, count, 128):
        spread = jnp.broadcast_to(row[:, first : first + 128], (128, 128))
        columns.append(jnp.sum(jnp.where(eye, spread, 0.0), axis=1, keepdims=True))
    return jnp.concatenate(columns, axis=0)


def slot_places(index):
    whole = index.astype(i32)
    return whole >> 8, whole & 255


def build_choosers(rows, pick_ref, put_ref):
    devices, capacity = rows.shape
    lines = pick_ref.shape[1]
    along = iota((devices, lines), 1)
    for rank in range(capacity):
        pick_ref[rank * devices : (rank + 1) * devices, :] = one_hot(rows[:, rank : rank + 1] == along)
    rows_float = rows.astype(f32)
    down = iota((lines, 128), 0).astype(f32)
    group = 128 // devices
    for rank in range(0, capacity, group):
        column = jnp.concatenate([rows_float[:, rank + k : rank + k + 1] for k in range(group)], axis=0)
        put_ref[:, rank * devices : rank * devices + 128] = one_hot(down == to_row(column))


def tissue_gather(values, pick_ref, columns):
    devices, capacity = columns.shape
    pieces = parts(values)
    width = values.shape[1]
    along = iota((devices, width), 1)
    slots = iota((devices, capacity), 1)
    result = jnp.zeros((devices, capacity), f32)
    group = 4
    for rank in range(0, capacity, group):
        taken = exact_dot(pick_ref[rank * devices : (rank + group) * devices, :], pieces)
        for k in range(group):
            here = taken[k * devices : (k + 1) * devices]
            hit = columns[:, rank + k : rank + k + 1] == along
            value = jnp.sum(jnp.where(hit, here, 0.0), axis=1, keepdims=True)
            result = jnp.where(slots == rank + k, value, result)
    return result


def tissue_scatter(current, put_ref, columns, width):
    devices, capacity = columns.shape
    along = iota((devices, width), 1)
    pieces = []
    for piece in parts(current):
        piece = piece.astype(f32)
        pieces.append(
            jnp.concatenate(
                [
                    jnp.where(columns[:, rank : rank + 1] == along, piece[:, rank : rank + 1], 0.0)
                    for rank in range(capacity)
                ],
                axis=0,
            ).astype(bf16)
        )
    return exact_dot(put_ref[...], pieces)


def store_faces(values_ref, side, low_ref, high_ref, across_ref):
    cells_x, cells_y, cells_z = values_ref.shape
    low_ref[...] = values_ref[0]
    high_ref[...] = values_ref[cells_x - 1]
    first = side == 1
    for x in range(cells_x):
        top = values_ref[x, 0:1, :]
        bottom = values_ref[x, cells_y - 1 : cells_y, :]
        across_ref[x : x + 1, :] = jnp.where(first, top, bottom)


def face_shapes(shape):
    x, y, z = shape
    return [sds((y, z)), sds((y, z)), sds((x, z))]


def halo_rows(across, side):
    low = jnp.where(side == 1, across, 0.0)
    high = jnp.where(side == 0, across, 0.0)
    return low, high


def shift_up_y(slab, high):
    rolled = pltpu.roll(slab, slab.shape[0] - 1, 0)
    return jnp.where(iota(slab.shape, 0) == slab.shape[0] - 1, high, rolled)


def shift_down_y(slab, low):
    return jnp.where(iota(slab.shape, 0) == 0, low, pltpu.roll(slab, 1, 0))


def shift_up_z(slab):
    return pltpu.roll(slab, slab.shape[1] - 1, 1)


def shift_down_z(slab):
    return pltpu.roll(slab, 1, 1)


def each_slab(count, step, first_carry):
    carry = first_carry
    carry = lax.fori_loop(0, count - 1, lambda x, c: step(x, c, False), carry)
    return step(count - 1, carry, True)


def coefficient_kernel(
    scal, volt, cond, mask, x_low, x_high, across, gx_o, gxl_o, gy_o, gyl_o, gz_o, next_o
):
    side = scal[0]
    cells_x, cells_y, cells_z = volt.shape
    last_lane = iota((cells_y, cells_z), 1) == cells_z - 1

    def face(a, ma, b, mb):
        return 0.5 * (a + b) * (ma * mb)

    low_flux_g = face(x_low[1], x_low[2], cond[0], mask[0].astype(f32))
    gxl_o[...] = low_flux_g

    def step(x, carry, last):
        v = volt[x]
        c = cond[x]
        m = mask[x].astype(f32)
        if last:
            vn, cn, mn = x_high[0], x_high[1], x_high[2]
        else:
            vn, cn, mn = volt[x + 1], cond[x + 1], mask[x + 1].astype(f32)
        gx = face(c, m, cn, mn)
        gx_o[x] = gx
        vl, vh = halo_rows(across[0, pl.ds(x, 1), :], side)
        cl, ch = halo_rows(across[1, pl.ds(x, 1), :], side)
        ml, mh = halo_rows(across[2, pl.ds(x, 1), :], side)
        gy = face(c, m, shift_up_y(c, ch), shift_up_y(m, mh))
        gyl = face(c[0:1], m[0:1], cl, ml)
        gz = jnp.where(last_lane, 0.0, face(c, m, shift_up_z(c), shift_up_z(m)))
        gy_o[x] = gy
        gyl_o[pl.ds(x, 1), :] = gyl
        gz_o[x] = gz
        fx = gx * (vn - v)
        fy = gy * (shift_up_y(v, vh) - v)
        fyl = gyl * (v[0:1] - vl)
        fz = gz * (shift_up_z(v) - v)
        total = fx - carry + fy - shift_down_y(fy, fyl) + fz - shift_down_z(fz)
        next_o[x] = v + time_step * (total + ionic(v))
        return fx

    each_slab(cells_x, step, low_flux_g * (volt[0] - x_low[0]))


def forward_kernel(scal, volt, gx, gxl, gy, gyl, gz, x_low, x_high, across, next_o):
    side = scal[0]
    cells_x = volt.shape[0]

    def step(x, carry, last):
        v = volt[x]
        vn = x_high[...] if last else volt[x + 1]
        vl, vh = halo_rows(across[pl.ds(x, 1), :], side)
        fx = gx[x] * (vn - v)
        fy = gy[x] * (shift_up_y(v, vh) - v)
        fyl = gyl[pl.ds(x, 1), :] * (v[0:1] - vl)
        fz = gz[x] * (shift_up_z(v) - v)
        total = fx - carry + fy - shift_down_y(fy, fyl) + fz - shift_down_z(fz)
        next_o[x] = v + time_step * (total + ionic(v))
        return fx

    each_slab(cells_x, step, gxl[...] * (volt[0] - x_low[...]))


def adjoint_kernel(first, *refs):
    scal, lam, volt, mask, gx, gxl, gy, gyl, gz = refs[:9]
    lam_low, lam_high, lam_across, v_low, v_high, v_across, m_low, m_high, m_across = refs[9:18]
    if first:
        next_o, grad_o = refs[18:]
    else:
        grad_i, next_o, grad_o = refs[18:]
    side = scal[0]
    cells_x, cells_y, cells_z = volt.shape
    last_lane = iota((cells_y, cells_z), 1) == cells_z - 1

    def step(x, carry, last):
        flux_before, product_before = carry
        a = lam[x]
        v = volt[x]
        m = mask[x].astype(f32)
        if last:
            an, vn, mn = lam_high[...], v_high[...], m_high[...]
        else:
            an, vn, mn = lam[x + 1], volt[x + 1], mask[x + 1].astype(f32)
        al, ah = halo_rows(lam_across[pl.ds(x, 1), :], side)
        vl, vh = halo_rows(v_across[pl.ds(x, 1), :], side)
        ml, mh = halo_rows(m_across[pl.ds(x, 1), :], side)
        dx = an - a
        fx = gx[x] * dx
        px = (m * mn) * dx * (vn - v)
        dy = shift_up_y(a, ah) - a
        fy = gy[x] * dy
        py = (m * shift_up_y(m, mh)) * dy * (shift_up_y(v, vh) - v)
        dyl = a[0:1] - al
        fyl = gyl[pl.ds(x, 1), :] * dyl
        pyl = (m[0:1] * ml) * dyl * (v[0:1] - vl)
        dz = shift_up_z(a) - a
        fz = gz[x] * dz
        pz = jnp.where(last_lane, 0.0, (m * shift_up_z(m)) * dz * (shift_up_z(v) - v))
        total = fx - flux_before + fy - shift_down_y(fy, fyl) + fz - shift_down_z(fz)
        products = px + product_before + py + shift_down_y(py, pyl) + pz + shift_down_z(pz)
        next_o[x] = a + time_step * (total + slope(v) * a)
        grad = (-0.5 * time_step) * products
        grad_o[x] = grad if first else grad_i[x] + grad
        return fx, px

    low_d = lam[0] - lam_low[...]
    low_p = (mask[0].astype(f32) * m_low[...]) * low_d * (volt[0] - v_low[...])
    each_slab(cells_x, step, (gxl[...] * low_d, low_p))


def unpack_info(info):
    names = ("device", "rank", "segment", "node", "sigma", "parent")
    return {name: info[:, k : k + 1] for k, name in enumerate(names)}


def slots_out(column, info, row_info, devices, capacity):
    put = one_hot(iota((devices, column.shape[0]), 0).astype(f32) == row_info[0:1, :])
    chosen = info["rank"] == iota((1, capacity), 1).astype(f32)
    pieces = [jnp.where(chosen, piece.astype(f32), 0.0).astype(bf16) for piece in parts(column)]
    return exact_dot(put, pieces)


def slots_in(slots, info):
    devices, capacity = slots.shape
    pick = one_hot(info["device"] == iota((1, devices), 1).astype(f32))
    taken = exact_dot(pick, parts(slots))
    chosen = info["rank"] == iota((1, capacity), 1).astype(f32)
    return jnp.sum(jnp.where(chosen, taken, 0.0), axis=1, keepdims=True)


def node_gather(values, info):
    segments, nodes = values.shape
    pick = one_hot(info["segment"] == iota((1, segments), 1).astype(f32))
    taken = exact_dot(pick, parts(values))
    chosen = info["node"] == iota((1, nodes), 1).astype(f32)
    return jnp.sum(jnp.where(chosen, taken, 0.0), axis=1, keepdims=True)


def node_scatter(column, info, row_info, segments, nodes):
    put = one_hot(iota((segments, 1), 0).astype(f32) == row_info[1:2, :])
    chosen = info["node"] == iota((1, nodes), 1).astype(f32)
    pieces = [jnp.where(chosen, piece.astype(f32), 0.0).astype(bf16) for piece in parts(column)]
    return exact_dot(put, pieces)


def lane_differences(values):
    nodes = values.shape[1]
    inside = iota(values.shape, 1) < nodes - 1
    return jnp.where(inside, pltpu.roll(values, nodes - 1, 1) - values, 0.0)


def window_pick(info, window):
    places = iota((1, window.shape[1]), 1).astype(f32)
    return jnp.sum(jnp.where(info["parent"] == places, window, 0.0), axis=1, keepdims=True)


def cable_flux(values, differences, info, tails, heads, child_sigma, child_parent):
    segments, nodes = values.shape
    edge = info["sigma"] * differences
    result = edge - pltpu.roll(edge, 1, 1)
    parent_tail = window_pick(info, tails)
    own_head = values[:, 0:1]
    own_tail = values[:, nodes - 1 : nodes]
    head_flux = jnp.where(info["parent"] >= 0.0, info["sigma"] * (parent_tail - own_head), 0.0)
    mine = child_parent == iota((segments, 1), 0).astype(f32)
    inflow = jnp.sum(
        jnp.where(mine, child_sigma * (heads - own_tail), 0.0), axis=1, keepdims=True
    )
    lane = iota(values.shape, 1)
    result = result + jnp.where(lane == 0, head_flux, 0.0)
    result = result + jnp.where(lane == nodes - 1, inflow, 0.0)
    return result, parent_tail


def family(first, tails, heads, children):
    tail_row = jnp.concatenate([t[...] for t in tails], axis=1)
    head_row = jnp.concatenate([h[0:1, :] for h in heads], axis=1)
    sigma_row = jnp.concatenate([c[1:2, :] for c in children], axis=1)
    parent_row = jnp.concatenate([c[2:3, :] for c in children], axis=1) - first.astype(f32)
    return tail_row, head_row, sigma_row, parent_row


def setup_kernel(
    plane, cells_y, cells_z, cells_x, grid_y, scal, voxel, node, parent, sigma, cable,
    slots_o, info_o, rows_o, tail_o, child_o,
):
    segments, nodes = cable.shape
    count = voxel.shape[1]
    devices, _, width = slots_o.shape
    capacity = width // 2
    first = scal[1]
    vox = voxel[...]
    coord_x = vox // plane
    inside = vox - coord_x * plane
    coord_y = inside // cells_z
    coord_z = inside - coord_y * cells_z
    block_x = coord_x // cells_x
    block_y = coord_y // cells_y
    device = (block_x * grid_y + block_y).astype(f32)
    local = ((coord_x - block_x * cells_x) * cells_y + coord_y - block_y * cells_y) * cells_z + coord_z
    spot = node[...] - first * nodes
    segment = spot // nodes
    lane = (spot - segment * nodes).astype(f32)
    segment = segment.astype(f32)
    own_parent = parent[...]
    relative = jnp.where(own_parent >= 0, (own_parent - first + 2 * segments).astype(f32), FAR)
    device_column = to_column(device)
    earlier = iota((count, count), 1) < iota((count, count), 0)
    same = (device_column == device) & earlier
    rank = jnp.sum(jnp.where(same, 1.0, 0.0), axis=1, keepdims=True)
    columns = [
        device_column,
        rank,
        to_column(segment),
        to_column(lane),
        to_column(sigma[...]),
        to_column(relative),
    ]
    spread = jnp.zeros((segments, 128), f32)
    where = iota((segments, 128), 1)
    for k, column in enumerate(columns):
        spread = jnp.where(where == k, column, spread)
    info_o[...] = spread
    rows_o[...] = jnp.zeros(rows_o.shape, f32)
    rows_o[0:1, :] = device
    rows_o[1:2, :] = segment
    info = unpack_info(spread)
    row_info = rows_o[...]
    value = node_gather(cable[...], info)
    index = slots_out(to_column((local + 1).astype(f32)), info, row_info, devices, capacity) - 1.0
    slots_o[:, 0, 0:capacity] = index
    slots_o[:, 0, capacity:width] = slots_out(value, info, row_info, devices, capacity)
    tail_o[...] = to_row(cable[:, nodes - 1 : nodes])
    child_o[0:1, :] = to_row(cable[:, 0:1])
    child_o[1:2, :] = sigma[...]
    child_o[2:3, :] = jnp.where(own_parent >= 0, own_parent.astype(f32), FAR)


def cable_start_kernel(
    scal, cable, info_i, t2, t1, t0, h0, h1, h2, next_o, parent_o
):
    info = unpack_info(info_i[...])
    u = cable[...]
    rows = family(scal[1], (t2, t1, t0), (h0, h1, h2), (h0, h1, h2))
    flux, parent_tail = cable_flux(u, lane_differences(u), info, *rows)
    next_o[...] = u + time_step * (flux + ionic(u))
    parent_o[...] = to_row(parent_tail)


def tissue_first_kernel(
    scal, slots, volt, partial, pick_o, put_o, next_o, sent_o, low_o, high_o, across_o
):
    devices, _, width = slots.shape
    capacity = width // 2
    cells_x, cells_y, cells_z = volt.shape
    lines = cells_x * cells_y
    index = slots[:, 0, 0:capacity]
    there = slots[:, 0, capacity:width]
    rows, columns = slot_places(index)
    build_choosers(rows, pick_o, put_o)
    here = tissue_gather(volt[...].reshape(lines, cells_z), pick_o, columns)
    current = jnp.where(rows >= 0, gap_conductance * (there - here), 0.0)
    added = tissue_scatter(current, put_o, columns, cells_z)
    after = partial[...].reshape(lines, cells_z) + time_step * added
    next_o[...] = after.reshape(volt.shape)
    sent_o[:, 0, 0:capacity] = here
    sent_o[:, 0, capacity:width] = tissue_gather(after, pick_o, columns)
    store_faces(next_o, scal[0], low_o, high_o, across_o)


def cable_first_kernel(
    scal, slots, cable, partial, info_i, rows_i, next_o, sent_o, there_o, tail_o, head_o
):
    devices, _, width = slots.shape
    capacity = width // 2
    info = unpack_info(info_i[...])
    row_info = rows_i[...]
    u = cable[...]
    segments, nodes = u.shape
    before = slots_in(slots[:, 0, 0:capacity], info)
    current = gap_conductance * (node_gather(u, info) - before)
    after = partial[...] - time_step * node_scatter(current, info, row_info, segments, nodes)
    next_o[...] = after
    sent_o[:, 0, :] = slots_out(node_gather(after, info), info, row_info, devices, capacity)
    there_o[...] = to_row(slots_in(slots[:, 0, capacity:width], info))
    tail_o[...] = to_row(after[:, nodes - 1 : nodes])
    head_o[...] = to_row(after[:, 0:1])


def cable_second_kernel(
    devices, capacity,
    scal, cable, target, there, info_i, rows_i, t2, t1, t0, h0, h1, h2, c0, c1, c2,
    next_o, adjoint_o, sent_o, parent_o, tail_o, head_o,
):
    info = unpack_info(info_i[...])
    row_info = rows_i[...]
    u = cable[...]
    segments, nodes = u.shape
    rows = family(scal[1], (t2, t1, t0), (h0, h1, h2), (c0, c1, c2))
    flux, parent_tail = cable_flux(u, lane_differences(u), info, *rows)
    current = gap_conductance * (node_gather(u, info) - to_column(there[...]))
    drawn = node_scatter(current, info, row_info, segments, nodes)
    after = u + time_step * (flux + ionic(u) - drawn)
    next_o[...] = after
    adjoint = loss_weight * (after - (1.0 - target[...].astype(f32) / target_span))
    adjoint_o[...] = adjoint
    sent_o[...] = slots_out(node_gather(adjoint, info), info, row_info, devices, capacity)
    parent_o[...] = to_row(parent_tail)
    tail_o[...] = to_row(adjoint[:, nodes - 1 : nodes])
    head_o[...] = to_row(adjoint[:, 0:1])


def tissue_second_kernel(
    scal, slots, before, first_slots, cable_sent, partial, mask, target, pick, put,
    next_o, adjoint_o, sent_o, low_o, high_o, across_o,
):
    capacity = slots.shape[2]
    cells_x, cells_y, cells_z = partial.shape
    lines = cells_x * cells_y
    rows, columns = slot_places(first_slots[:, 0, 0:capacity])
    there = slots[:, 0, :]
    here = before[:, 0, capacity : 2 * capacity]
    current = jnp.where(rows >= 0, gap_conductance * (there - here), 0.0)
    added = tissue_scatter(current, put, columns, cells_z)
    after = partial[...] + time_step * added.reshape(partial.shape)
    next_o[...] = after
    adjoint = (
        loss_weight
        * mask[...].astype(f32)
        * (after - (1.0 - target[...].astype(f32) / target_span))
    )
    adjoint_o[...] = adjoint
    sent_o[:, 0, 0:capacity] = tissue_gather(adjoint.reshape(lines, cells_z), pick, columns)
    sent_o[:, 0, capacity : 2 * capacity] = cable_sent[...]
    store_faces(adjoint_o, scal[0], low_o, high_o, across_o)


def cable_adjoint_kernel(first, *refs):
    scal, adjoint, old, parent_old, info_i = refs[:5]
    t2, t1, t0, h0, h1, h2, c0, c1, c2 = refs[5:14]
    if first:
        next_o, grad_o = refs[14:]
    else:
        grad_i, next_o, grad_o = refs[14:]
    info = unpack_info(info_i[...])
    mu = adjoint[...]
    u = old[...]
    rows = family(scal[1], (t2, t1, t0), (h0, h1, h2), (c0, c1, c2))
    differences = lane_differences(mu)
    flux, parent_tail = cable_flux(mu, differences, info, *rows)
    next_o[...] = mu + time_step * (flux + slope(u) * mu)
    inner = jnp.sum(differences * lane_differences(u), axis=1, keepdims=True)
    head = (mu[:, 0:1] - parent_tail) * (to_column(parent_old[...]) - u[:, 0:1])
    grad = time_step * (jnp.where(info["parent"] >= 0.0, head, 0.0) - inner)
    grad = to_row(grad)
    grad_o[...] = grad if first else grad_i[...] + grad


def exchange_kernel(last, *refs):
    (scal, slots, sent, first_slots, tissue_partial, cable_partial, info_i, rows_i, pick, put) = refs[:10]
    outs = refs[10:]
    devices, _, width = slots.shape
    capacity = width // 2
    cells_x, cells_y, cells_z = tissue_partial.shape
    lines = cells_x * cells_y
    segments, nodes = cable_partial.shape
    rows, columns = slot_places(first_slots[:, 0, 0:capacity])
    tissue_here = sent[:, 0, 0:capacity]
    cable_here = sent[:, 0, capacity:width]
    tissue_there = slots[:, 0, 0:capacity]
    cable_there = slots[:, 0, capacity:width]
    info = unpack_info(info_i[...])
    row_info = rows_i[...]
    current = jnp.where(rows >= 0, gap_conductance * (cable_there - tissue_here), 0.0)
    added = tissue_scatter(current, put, columns, cells_z)
    tissue_after = tissue_partial[...] + time_step * added.reshape(tissue_partial.shape)
    outs[0][...] = tissue_after
    drawn = slots_in(gap_conductance * (cable_here - tissue_there), info)
    cable_after = cable_partial[...] - time_step * node_scatter(drawn, info, row_info, segments, nodes)
    outs[1][...] = cable_after
    if not last:
        sent_o, low_o, high_o, across_o, tail_o, head_o = outs[2:]
        sent_o[:, 0, 0:capacity] = tissue_gather(tissue_after.reshape(lines, cells_z), pick, columns)
        sent_o[:, 0, capacity:width] = slots_out(
            node_gather(cable_after, info), info, row_info, devices, capacity
        )
        store_faces(outs[0], scal[0], low_o, high_o, across_o)
        tail_o[...] = to_row(cable_after[:, nodes - 1 : nodes])
        head_o[...] = to_row(cable_after[:, 0:1])


def shifted(block, distance):
    axes = ("gx", "gy")
    devices = range(lax.axis_size(axes))
    return lax.ppermute(block, axes, [(i - distance, i) for i in devices if i - distance in devices])


def tissue_halo(low, high, across, x_dims=None):
    size = lax.axis_size("gx")
    up = [(i, i + 1) for i in range(size - 1)]
    from_low = lax.ppermute(high, "gx", up)
    from_high = lax.ppermute(low, "gx", [(b, a) for a, b in up])
    beside = lax.ppermute(across, "gy", [(0, 1), (1, 0)])
    return from_low, from_high, beside


def cable_halo(tails, heads):
    return (shifted(tails, 2), shifted(tails, 1)), (shifted(heads, -1), shifted(heads, -2))


def swap_slots(slots):
    return lax.all_to_all(slots, ("gx", "gy"), split_axis=0, concat_axis=0, tiled=True)


def body(
    initial_voltage,
    conductivity,
    tissue_mask,
    target_step,
    initial_purkinje,
    purkinje_conductivity,
    segment_parent,
    purkinje_target,
    junction_voxel,
    junction_node,
):
    shape = initial_voltage.shape
    cells_x, cells_y, cells_z = shape
    segments, nodes = initial_purkinje.shape
    grid_x, grid_y = lax.axis_size("gx"), lax.axis_size("gy")
    devices = grid_x * grid_y
    per_device = junction_voxel.shape[0]
    capacity = max(2, 2 * per_device // devices)
    slots = devices * capacity
    lines = cells_x * cells_y
    plane = cells_y * grid_y * cells_z
    side = lax.axis_index("gy")
    first = lax.axis_index(("gx", "gy")) * segments
    scal = jnp.stack([side, first]).astype(i32)
    one = sds((1, segments))
    cable_shape = sds((segments, nodes))
    tissue_shape = sds(shape)
    double = sds((devices, 1, 2 * capacity))

    sent0, info, rows, tail0, child0 = call(
        functools.partial(setup_kernel, plane, cells_y, cells_z, cells_x, grid_y),
        "setup",
        [double, sds((segments, 128)), sds((8, segments)), one, sds((3, segments))],
        scal,
        junction_voxel.reshape(1, -1),
        junction_node.reshape(1, -1),
        segment_parent.reshape(1, -1),
        purkinje_conductivity.reshape(1, -1),
        initial_purkinje,
    )
    arrived0 = swap_slots(sent0)

    def faces(array):
        return array[0], array[cells_x - 1], jnp.where(side == 1, array[:, 0], array[:, cells_y - 1])

    faced = [faces(a) for a in (initial_voltage, conductivity, tissue_mask.astype(f32))]
    edge0 = tissue_halo(*[jnp.stack([f[k] for f in faced]) for k in range(3)])
    gx, gxl, gy, gyl, gz, part1 = call(
        coefficient_kernel,
        "coefficients",
        [tissue_shape, sds((cells_y, cells_z)), tissue_shape, sds((cells_x, cells_z)), tissue_shape, tissue_shape],
        scal,
        initial_voltage,
        conductivity,
        tissue_mask,
        *edge0,
        flops=20_000_000,
    )
    conduct = (gx, gxl, gy, gyl, gz)
    mask_edge = tuple(e[2] for e in edge0)
    volt_edge0 = tuple(e[0] for e in edge0)

    (tails2, tails1), (heads1, heads2) = cable_halo(tail0, child0)
    children = (child0, heads1, heads2)
    cable_part1, parent0 = call(
        cable_start_kernel,
        "cable_start",
        [cable_shape, one],
        scal,
        initial_purkinje,
        info,
        tails2,
        tails1,
        tail0,
        *children,
    )

    choosers = [sds((slots, lines), bf16), sds((lines, slots), bf16)]
    pick, put, voltage1, sent1, *faces1 = call(
        tissue_first_kernel,
        "tissue_first",
        choosers + [tissue_shape, double] + face_shapes(shape),
        scal,
        arrived0,
        initial_voltage,
        part1,
        flops=20_000_000,
    )
    arrived1 = swap_slots(sent1)
    edge1 = tissue_halo(*faces1)
    (part2,) = call(
        forward_kernel, "forward", [tissue_shape], scal, voltage1, *conduct, *edge1, flops=20_000_000
    )

    cable1, sent2, there1, tail1, head1 = call(
        cable_first_kernel,
        "cable_first",
        [cable_shape, sds((devices, 1, capacity)), one, one, one],
        scal,
        arrived1,
        initial_purkinje,
        cable_part1,
        info,
        rows,
    )
    arrived2 = swap_slots(sent2)
    (tails2, tails1), (heads1, heads2) = cable_halo(tail1, head1)
    cable2, mu2, cable_sent, parent1, tail2, head2 = call(
        functools.partial(cable_second_kernel, devices, capacity),
        "cable_second",
        [cable_shape, cable_shape, sds((devices, capacity)), one, one, one],
        scal,
        cable1,
        purkinje_target,
        there1,
        info,
        rows,
        tails2,
        tails1,
        tail1,
        head1,
        heads1,
        heads2,
        *children,
    )

    voltage2, lam2, sent3, *faces2 = call(
        tissue_second_kernel,
        "tissue_second",
        [tissue_shape, tissue_shape, double] + face_shapes(shape),
        scal,
        arrived2,
        sent1,
        arrived0,
        cable_sent,
        part2,
        tissue_mask,
        target_step,
        pick,
        put,
    )

    def adjoint(lam, lam_edge, volt, volt_edge, mu, tail, head, old, parent_old, grads):
        is_first = grads is None
        lam_part, grad = call(
            functools.partial(adjoint_kernel, is_first),
            "adjoint",
            [tissue_shape, tissue_shape],
            scal,
            lam,
            volt,
            tissue_mask,
            *conduct,
            *lam_edge,
            *volt_edge,
            *mask_edge,
            *([] if is_first else [grads[0]]),
            flops=30_000_000,
        )
        (b2, b1), (a1, a2) = cable_halo(tail, head)
        mu_part, cable_grad = call(
            functools.partial(cable_adjoint_kernel, is_first),
            "cable_adjoint",
            [cable_shape, one],
            scal,
            mu,
            old,
            parent_old,
            info,
            b2,
            b1,
            tail,
            head,
            a1,
            a2,
            *children,
            *([] if is_first else [grads[1]]),
        )
        return lam_part, mu_part, (grad, cable_grad)

    def exchange(last, arrived, sent, lam_part, mu_part):
        outs = [tissue_shape, cable_shape]
        if not last:
            outs += [double] + face_shapes(shape) + [one, one]
        return call(
            functools.partial(exchange_kernel, last),
            "exchange",
            outs,
            scal,
            arrived,
            sent,
            arrived0,
            lam_part,
            mu_part,
            info,
            rows,
            pick,
            put,
        )

    arrived3 = swap_slots(sent3)
    edge2 = tissue_halo(*faces2)
    lam_part, mu_part, grads = adjoint(
        lam2, edge2, voltage1, edge1, mu2, tail2, head2, cable1, parent1, None
    )
    lam1, mu1, sent4, low3, high3, across3, tail3, head3 = exchange(
        False, arrived3, sent3, lam_part, mu_part
    )
    arrived4 = swap_slots(sent4)
    edge3 = tissue_halo(low3, high3, across3)
    lam_part, mu_part, grads = adjoint(
        lam1, edge3, initial_voltage, volt_edge0, mu1, tail3, head3, initial_purkinje, parent0, grads
    )
    lam0, mu0 = exchange(True, arrived4, sent4, lam_part, mu_part)
    return (voltage2, cable2, grads[0], grads[1].reshape(-1), lam0, mu0)


def solution(mesh):
    tissue = P(("groups", "gx"), "gy", None)
    cable = P(("groups", "gx", "gy"), None)
    flat = P(("groups", "gx", "gy"))
    in_specs = (tissue, tissue, tissue, tissue, cable, flat, flat, cable, flat, flat)
    out_specs = (tissue, cable, tissue, flat, tissue, cable)
    return jax.shard_map(body, mesh=mesh, in_specs=in_specs, out_specs=out_specs, check_vma=False)
```

```python
import functools

import jax
import jax.numpy as jnp
from jax import lax
from jax.experimental import pallas as pl
from jax.experimental.pallas import tpu as pltpu
from jax.sharding import PartitionSpec as P

time_step = 0.05
gap_conductance = 4.0
ion_rate = 8.0
threshold = 0.15
loss_weight = 10.0
target_span = 8.0

INTERPRET = False
f32 = jnp.float32
bf16 = jnp.bfloat16
i32 = jnp.int32
FAR = -1.0e7
LIMIT = 60 << 20


def sds(shape, dtype=f32):
    return jax.ShapeDtypeStruct(shape, dtype)

DMA = pltpu.SemaphoreType.DMA


def call(kernel, name, outs, arrays, scratch=(), scalars=None, flops=20_000_000):
    def spec(inside):
        return pl.BlockSpec(memory_space=pltpu.VMEM if inside else pl.ANY)

    specs = [pl.BlockSpec(memory_space=pltpu.SMEM)] if scalars is not None else []
    specs += [spec(inside) for _, inside in arrays]
    args = ([scalars] if scalars is not None else []) + [a for a, _ in arrays]
    return pl.pallas_call(
        kernel,
        name=name,
        out_shape=[o for o, _ in outs],
        in_specs=specs,
        out_specs=[spec(inside) for _, inside in outs],
        scratch_shapes=list(scratch),
        compiler_params=pltpu.CompilerParams(vmem_limit_bytes=LIMIT),
        cost_estimate=pl.CostEstimate(flops=flops, transcendentals=0, bytes_accessed=4_000_000),
        interpret=INTERPRET,
    )(*args)


def near(*arrays):
    return [(a, True) for a in arrays]


def far(*arrays):
    return [(a, False) for a in arrays]


def copy(source, target, sem):
    started = pltpu.make_async_copy(source, target, sem)
    started.start()
    return started


def ionic(values):
    return ion_rate * values * (values - threshold) * (1.0 - values)


def slope(values):
    return ion_rate * (-3.0 * values * values + 2.0 * (1.0 + threshold) * values - threshold)


def iota(shape, dim):
    return lax.broadcasted_iota(i32, shape, dim)


def parts(values):
    high = values.astype(bf16)
    return high, (values - high.astype(f32)).astype(bf16)


def parts_dot(chooser, pieces):
    total = None
    for piece in pieces:
        term = jnp.dot(chooser, piece, preferred_element_type=f32)
        total = term if total is None else total + term
    return total


def exact_parts(values):
    high = values.astype(bf16)
    rest = values - high.astype(f32)
    middle = rest.astype(bf16)
    return high, middle, (rest - middle.astype(f32)).astype(bf16)


def one_hot(test):
    return jnp.where(test, 1.0, 0.0).astype(bf16)


def to_row(column):
    count = column.shape[0]
    eye = iota((128, 128), 0) == iota((128, 128), 1)
    rows = []
    for first in range(0, count, 128):
        spread = jnp.broadcast_to(column[first : first + 128], (128, 128))
        rows.append(jnp.sum(jnp.where(eye, spread, 0.0), axis=0, keepdims=True))
    return jnp.concatenate(rows, axis=1)


def to_column(row):
    count = row.shape[1]
    eye = iota((128, 128), 0) == iota((128, 128), 1)
    columns = []
    for first in range(0, count, 128):
        spread = jnp.broadcast_to(row[:, first : first + 128], (128, 128))
        columns.append(jnp.sum(jnp.where(eye, spread, 0.0), axis=1, keepdims=True))
    return jnp.concatenate(columns, axis=0)


def put_line(ref, place, row):
    width = ref.shape[1]
    for k in range(row.shape[1] // width):
        ref[place + k : place + k + 1, :] = row[:, k * width : (k + 1) * width]


def get_line(ref, place, length):
    width = ref.shape[1]
    return jnp.concatenate([ref[place + k : place + k + 1, :] for k in range(length // width)], axis=1)


def spread_slots(table, ref):
    devices, capacity = table.shape
    for rank in range(capacity):
        ref[rank * devices : (rank + 1) * devices, :] = jnp.broadcast_to(
            table[:, rank : rank + 1], (devices, 128)
        )


def place_slots(index, cells_z, line_ref, lane_ref, row_ref):
    whole = index.astype(i32)
    line = whole // cells_z
    lane = whole - line * cells_z
    line = jnp.where(whole < 0, -1, line)
    spread_slots(line.astype(f32), line_ref)
    spread_slots(lane.astype(f32), lane_ref)
    slots = line_ref.shape[0]
    eye = iota((128, 128), 0) == iota((128, 128), 1)
    for first in range(0, slots, 128):
        block = jnp.where(eye, line_ref[first : first + 128, :], 0.0)
        row_ref[:, first : first + 128] = jnp.sum(block, axis=0, keepdims=True)


def split_field(values_ref, high_ref, low_ref):
    cells_x, cells_y, _ = values_ref.shape

    def step(x, _):
        high, low = parts(values_ref[x])
        high_ref[pl.ds(x * cells_y, cells_y), :] = high
        low_ref[pl.ds(x * cells_y, cells_y), :] = low
        return 0

    lax.fori_loop(0, cells_x, step, 0)


def tissue_gather(high_ref, low_ref, line_ref, lane_ref, value_ref, devices):
    slots = line_ref.shape[0]
    lines, width = high_ref.shape
    block = 256
    along = iota((block, 128), 1).astype(f32)

    def step(b, _):
        where = pl.ds(b * block, block)
        line = line_ref[where, :]
        lane = lane_ref[where, :]
        chooser = jnp.concatenate(
            [one_hot(line == along + float(first)) for first in range(0, lines, 128)], axis=1
        )
        taken = parts_dot(chooser, (high_ref[...], low_ref[...]))
        kept = jnp.zeros((block, 128), f32)
        for first in range(0, width, 128):
            kept = kept + jnp.where(lane == along + float(first), taken[:, first : first + 128], 0.0)
        value_ref[where, :] = jnp.broadcast_to(jnp.sum(kept, axis=1, keepdims=True), (block, 128))
        return 0

    lax.fori_loop(0, slots // block, step, 0)
    capacity = slots // devices
    table = jnp.zeros((devices, capacity), f32)
    which = iota((devices, capacity), 1)
    for rank in range(capacity):
        table = jnp.where(
            which == rank, value_ref[rank * devices : (rank + 1) * devices, 0:capacity], table
        )
    return table


def tissue_scatter(current, lane_ref, row_ref, value_ref, high_ref, low_ref, sum_ref):
    slots = lane_ref.shape[0]
    cells_x, cells_y, width = sum_ref.shape
    spread_slots(current, value_ref)
    along = iota((128, 128), 1).astype(f32)

    def build(b, _):
        where = pl.ds(b * 128, 128)
        lane = lane_ref[where, :]
        high, low = parts(value_ref[where, :])
        for first in range(0, width, 128):
            hit = lane == along + float(first)
            high_ref[where, first : first + 128] = jnp.where(hit, high.astype(f32), 0.0).astype(bf16)
            low_ref[where, first : first + 128] = jnp.where(hit, low.astype(f32), 0.0).astype(bf16)
        return 0

    lax.fori_loop(0, slots // 128, build, 0)
    slabs = 256 // cells_y
    down = iota((slabs * cells_y, slots), 0).astype(f32)

    def step(b, _):
        base = (b * slabs * cells_y).astype(f32)
        chooser = one_hot(down == row_ref[...] - base)
        added = parts_dot(chooser, (high_ref[...], low_ref[...]))
        sum_ref[pl.ds(b * slabs, slabs)] = added.reshape(slabs, cells_y, width)
        return 0

    lax.fori_loop(0, cells_x // slabs, step, 0)


def field_scratch(slots, shape):
    lines = shape[0] * shape[1]
    assert slots == lines
    wide = pltpu.VMEM((lines, shape[2]), bf16)
    return [
        pltpu.VMEM((slots, 128), f32),
        pltpu.VMEM((slots, 128), f32),
        pltpu.VMEM((1, slots), f32),
        pltpu.VMEM((slots, 128), f32),
        wide,
        wide,
        pltpu.VMEM(shape, f32),
    ]


def shift_up_y(slab, high):
    rolled = pltpu.roll(slab, slab.shape[0] - 1, 0)
    return jnp.where(iota(slab.shape, 0) == slab.shape[0] - 1, high, rolled)


def shift_down_y(slab, low):
    return jnp.where(iota(slab.shape, 0) == 0, low, pltpu.roll(slab, 1, 0))


def shift_up_z(slab):
    return pltpu.roll(slab, slab.shape[1] - 1, 1)


def shift_down_z(slab):
    return pltpu.roll(slab, 1, 1)


def face(a, b):
    return jnp.where(jnp.minimum(a, b) > 0.0, 0.5 * (a + b), 0.0)


def each_slab(count, step, first_carry):
    carry = lax.fori_loop(0, count - 1, lambda x, c: step(x, c, False), first_carry)
    return step(count - 1, carry, True)


def y_lines(low_ref, high_ref, place, x, side):
    low = jnp.where(side == 1.0, low_ref[pl.ds(place + x, 1), :], 0.0)
    high = jnp.where(side == 0.0, high_ref[pl.ds(place + x, 1), :], 0.0)
    return low, high


def forward_steps(v_ref, s_ref, v_edge, s_edge, side, finish):
    cells_x, cells_y, cells_z = v_ref.shape
    last_lane = iota((cells_y, cells_z), 1) == cells_z - 1
    vxl, vxh, vyl, vyh, vx, vy = v_edge
    sxl, sxh, syl, syh, sx, sy = s_edge

    def step(x, carry, last):
        v = v_ref[x]
        s = s_ref[x]
        if last:
            vn, sn = vxh[vx : vx + cells_y, :], sxh[sx : sx + cells_y, :]
        else:
            vn, sn = v_ref[x + 1], s_ref[x + 1]
        vl, vh = y_lines(vyl, vyh, vy, x, side)
        sl, sh = y_lines(syl, syh, sy, x, side)
        fx = face(s, sn) * (vn - v)
        fy = face(s, shift_up_y(s, sh)) * (shift_up_y(v, vh) - v)
        fyl = face(s[0:1], sl) * (v[0:1] - vl)
        fz = jnp.where(last_lane, 0.0, face(s, shift_up_z(s)) * (shift_up_z(v) - v))
        finish(x, v, s, fx - carry + fy - shift_down_y(fy, fyl) + fz - shift_down_z(fz))
        return fx

    low_v, low_s = vxl[vx : vx + cells_y, :], sxl[sx : sx + cells_y, :]
    each_slab(cells_x, step, face(s_ref[0], low_s) * (v_ref[0] - low_v))


def adjoint_steps(a_ref, v_ref, s_ref, a_edge, v_edge, s_edge, side, finish):
    cells_x, cells_y, cells_z = v_ref.shape
    last_lane = iota((cells_y, cells_z), 1) == cells_z - 1
    axl, axh, ayl, ayh, ax, ay = a_edge
    vxl, vxh, vyl, vyh, vx, vy = v_edge
    sxl, sxh, syl, syh, sx, sy = s_edge

    def pair(s, sn, d, e):
        both = jnp.minimum(s, sn) > 0.0
        d = jnp.where(both, d, 0.0)
        return (0.5 * (s + sn)) * d, d * e

    def step(x, carry, last):
        flux_before, product_before = carry
        a = a_ref[x]
        v = v_ref[x]
        s = s_ref[x]
        if last:
            an = axh[ax : ax + cells_y, :]
            vn = vxh[vx : vx + cells_y, :]
            sn = sxh[sx : sx + cells_y, :]
        else:
            an, vn, sn = a_ref[x + 1], v_ref[x + 1], s_ref[x + 1]
        al, ah = y_lines(ayl, ayh, ay, x, side)
        vl, vh = y_lines(vyl, vyh, vy, x, side)
        sl, sh = y_lines(syl, syh, sy, x, side)
        fx, px = pair(s, sn, an - a, vn - v)
        fy, py = pair(s, shift_up_y(s, sh), shift_up_y(a, ah) - a, shift_up_y(v, vh) - v)
        fyl, pyl = pair(s[0:1], sl, a[0:1] - al, v[0:1] - vl)
        dz = jnp.where(last_lane, 0.0, shift_up_z(a) - a)
        fz, pz = pair(s, shift_up_z(s), dz, shift_up_z(v) - v)
        flux = fx - flux_before + fy - shift_down_y(fy, fyl) + fz - shift_down_z(fz)
        product = px + product_before + py + shift_down_y(py, pyl) + pz + shift_down_z(pz)
        finish(x, a, v, flux, product)
        return fx, px

    low = [ref[at : at + cells_y, :] for ref, at in ((axl, ax), (vxl, vx), (sxl, sx))]
    each_slab(cells_x, step, pair(s_ref[0], low[2], a_ref[0] - low[0], v_ref[0] - low[1]))


def store_faces(values_ref, up2, dn2, up1, dn1):
    cells_x, cells_y, _ = values_ref.shape
    dn2[0:cells_y, :] = values_ref[0]
    up2[0:cells_y, :] = values_ref[cells_x - 1]
    for x in range(cells_x):
        dn1[x : x + 1, :] = values_ref[x, 0:1, :]
        up1[x : x + 1, :] = values_ref[x, cells_y - 1 : cells_y, :]


def store_ends(values, place_x, place_y, up2, dn2, up1, dn1):
    nodes = values.shape[1]
    tail = to_row(values[:, nodes - 1 : nodes])
    head = to_row(values[:, 0:1])
    put_line(up2, place_x, tail)
    put_line(up1, place_y, tail)
    put_line(dn2, place_x, head)
    put_line(dn1, place_y, head)


def unpack_info(info):
    names = ("device", "rank", "segment", "node", "sigma", "parent")
    return {name: info[:, k : k + 1] for k, name in enumerate(names)}


def slots_out(column, info, row_info, devices, capacity, split=parts):
    put = one_hot(iota((devices, column.shape[0]), 0).astype(f32) == row_info[0:1, :])
    chosen = info["rank"] == iota((1, capacity), 1).astype(f32)
    pieces = [jnp.where(chosen, piece.astype(f32), 0.0).astype(bf16) for piece in split(column)]
    return parts_dot(put, pieces)


def slots_in(slots, info):
    devices, capacity = slots.shape
    pick = one_hot(info["device"] == iota((1, devices), 1).astype(f32))
    taken = parts_dot(pick, parts(slots))
    chosen = info["rank"] == iota((1, capacity), 1).astype(f32)
    return jnp.sum(jnp.where(chosen, taken, 0.0), axis=1, keepdims=True)


def node_gather(values, info):
    segments, nodes = values.shape
    pick = one_hot(info["segment"] == iota((1, segments), 1).astype(f32))
    taken = parts_dot(pick, parts(values))
    chosen = info["node"] == iota((1, nodes), 1).astype(f32)
    return jnp.sum(jnp.where(chosen, taken, 0.0), axis=1, keepdims=True)


def node_scatter(column, info, row_info, segments, nodes):
    put = one_hot(iota((segments, 1), 0).astype(f32) == row_info[1:2, :])
    chosen = info["node"] == iota((1, nodes), 1).astype(f32)
    pieces = [jnp.where(chosen, piece.astype(f32), 0.0).astype(bf16) for piece in parts(column)]
    return parts_dot(put, pieces)


def lane_differences(values):
    nodes = values.shape[1]
    inside = iota(values.shape, 1) < nodes - 1
    return jnp.where(inside, pltpu.roll(values, nodes - 1, 1) - values, 0.0)


def window_pick(info, window):
    places = iota((1, window.shape[1]), 1).astype(f32)
    return jnp.sum(jnp.where(info["parent"] == places, window, 0.0), axis=1, keepdims=True)


def cable_flux(values, differences, info, tails, heads, child_sigma, child_parent):
    segments, nodes = values.shape
    edge = info["sigma"] * differences
    result = edge - pltpu.roll(edge, 1, 1)
    parent_tail = window_pick(info, tails)
    own_head = values[:, 0:1]
    own_tail = values[:, nodes - 1 : nodes]
    head_flux = jnp.where(info["parent"] >= 0.0, info["sigma"] * (parent_tail - own_head), 0.0)
    mine = child_parent == iota((segments, 1), 0).astype(f32)
    inflow = jnp.sum(
        jnp.where(mine, child_sigma * (heads - own_tail), 0.0), axis=1, keepdims=True
    )
    lane = iota(values.shape, 1)
    result = result + jnp.where(lane == 0, head_flux, 0.0)
    result = result + jnp.where(lane == nodes - 1, inflow, 0.0)
    return result, parent_tail


def join(rows):
    return jnp.concatenate(rows, axis=1)


def family(values, edge, first_own, first_edge, first_device, place_x, place_y):
    segments, nodes = values.shape
    up2, dn2, up1, dn1 = edge
    _, first_dn2, _, first_dn1 = first_edge
    tail = to_row(values[:, nodes - 1 : nodes])
    head = to_row(values[:, 0:1])
    lines = segments // up2.shape[1]
    fx = first_dn2.shape[0] - 8
    fy = first_dn1.shape[0] - 8
    tails = join([get_line(up2, place_x, segments), get_line(up1, place_y, segments), tail])
    heads = join([head, get_line(dn1, place_y, segments), get_line(dn2, place_x, segments)])
    both = []
    for k in (1, 2):
        both.append(
            join(
                [
                    get_line(first_own, fy + k * lines, segments),
                    get_line(first_dn1, fy + k * lines, segments),
                    get_line(first_dn2, fx + k * lines, segments),
                ]
            )
        )
    return tails, heads, both[0], both[1] - first_device


def setup_kernel(
    plane, cells_y, cells_z, cells_x, grid_y,
    scal, voxel, node, parent, sigma, cable, volt, cond, mask,
    slots_o, info_o, rows_o, up2, dn2, up1, dn1,
    face_v, face_c, face_m, row_v, row_c, row_m, sems,
):
    high = cells_y - 8
    started = []
    for k, (whole, faces, rows) in enumerate(
        ((volt, face_v, row_v), (cond, face_c, row_c), (mask, face_m, row_m))
    ):
        started.append(copy(whole.at[0], faces.at[0], sems.at[4 * k]))
        started.append(copy(whole.at[cells_x - 1], faces.at[1], sems.at[4 * k + 1]))
        started.append(copy(whole.at[:, pl.ds(0, 8), :], rows.at[0], sems.at[4 * k + 2]))
        started.append(copy(whole.at[:, pl.ds(high, 8), :], rows.at[1], sems.at[4 * k + 3]))
    segments, nodes = cable.shape
    count = voxel.shape[1]
    devices, _, width = slots_o.shape
    capacity = width // 2
    first = scal[1]
    vox = voxel[...]
    coord_x = vox // plane
    inside = vox - coord_x * plane
    coord_y = inside // cells_z
    coord_z = inside - coord_y * cells_z
    block_x = coord_x // cells_x
    block_y = coord_y // cells_y
    device = (block_x * grid_y + block_y).astype(f32)
    local = ((coord_x - block_x * cells_x) * cells_y + coord_y - block_y * cells_y) * cells_z + coord_z
    spot = node[...] - first * nodes
    segment = spot // nodes
    lane = (spot - segment * nodes).astype(f32)
    segment = segment.astype(f32)
    own_parent = parent[...]
    relative = jnp.where(own_parent >= 0, (own_parent - first + 2 * segments).astype(f32), FAR)
    device_column = to_column(device)
    earlier = iota((count, count), 1) < iota((count, count), 0)
    same = (device_column == device) & earlier
    rank = jnp.sum(jnp.where(same, 1.0, 0.0), axis=1, keepdims=True)
    columns = [
        device_column,
        rank,
        to_column(segment),
        to_column(lane),
        to_column(sigma[...]),
        to_column(relative),
        scal[0].astype(f32),
        first.astype(f32),
    ]
    spread = jnp.zeros((segments, 128), f32)
    where = iota((segments, 128), 1)
    for k, column in enumerate(columns):
        spread = jnp.where(where == k, column, spread)
    info_o[...] = spread
    rows_o[...] = jnp.zeros(rows_o.shape, f32)
    rows_o[0:1, :] = device
    rows_o[1:2, :] = segment
    info = unpack_info(spread)
    row_info = rows_o[...]
    value = node_gather(cable[...], info)
    index = slots_out(
        to_column((local + 1).astype(f32)), info, row_info, devices, capacity, exact_parts
    ) - 1.0
    slots_o[:, 0, 0:capacity] = index
    slots_o[:, 0, capacity:width] = slots_out(value, info, row_info, devices, capacity)
    place_x, place_y = 2 * cells_y, 2 * cells_x
    for ref, place in ((up2, place_x), (dn2, place_x), (up1, place_y), (dn1, place_y)):
        ref[place : place + 8, :] = jnp.zeros((8, cells_z), f32)
    store_ends(cable[...], place_x, place_y, up2, dn2, up1, dn1)
    lines = segments // cells_z
    plain_parent = jnp.where(own_parent >= 0, own_parent.astype(f32), FAR)
    for ref, place in ((dn2, place_x), (dn1, place_y)):
        put_line(ref, place + lines, sigma[...])
        put_line(ref, place + 2 * lines, plain_parent)
    for each in started:
        each.wait()
    for k, ref in ((0, dn2), (1, up2)):
        ref[0:cells_y, :] = face_v[k]
        ref[cells_y : 2 * cells_y, :] = face_c[k] * face_m[k].astype(f32)
    for k, at, ref in ((0, 0, dn1), (1, 7, up1)):
        for x in range(cells_x):
            ref[x : x + 1, :] = row_v[k, x, at : at + 1, :]
            ref[cells_x + x : cells_x + x + 1, :] = (
                row_c[k, x, at : at + 1, :] * row_m[k, x, at : at + 1, :].astype(f32)
            )


def first_edges(edge, cells_x, cells_y):
    up2, dn2, up1, dn1 = edge
    return (up2, dn2, up1, dn1, 0, 0), (up2, dn2, up1, dn1, cells_y, cells_x)


def tissue_first_kernel(
    slots, info_i, up2, dn2, up1, dn1, volt, cond, mask,
    next_h, soft_h, sent_o, out_up2, out_dn2, out_up1, out_dn1,
    line_r, lane_r, row_r, value_r, high_r, low_r, sum_r, v_r, c_r, m_r, next_r, sems,
):
    started = [copy(h, r, sems.at[k]) for k, (h, r) in enumerate(((volt, v_r), (cond, c_r), (mask, m_r)))]
    devices, _, width = slots.shape
    capacity = width // 2
    cells_x, cells_y, cells_z = volt.shape
    side = info_i[0:1, 6:7]
    index = slots[:, 0, 0:capacity]
    there = slots[:, 0, capacity:width]
    place_slots(index, cells_z, line_r, lane_r, row_r)
    for each in started:
        each.wait()

    def prepare(x, _):
        c_r[x] = c_r[x] * m_r[x].astype(f32)
        return 0

    lax.fori_loop(0, cells_x, prepare, 0)
    out_soft = copy(c_r, soft_h, sems.at[3])
    split_field(v_r, high_r, low_r)
    here = tissue_gather(high_r, low_r, line_r, lane_r, value_r, devices)
    current = jnp.where(index >= 0.0, gap_conductance * (there - here), 0.0)
    tissue_scatter(current, lane_r, row_r, value_r, high_r, low_r, sum_r)

    def finish(x, v, s, flux):
        after = v + time_step * (flux + ionic(v) + sum_r[x])
        next_r[x] = after
        high, low = parts(after)
        high_r[pl.ds(x * cells_y, cells_y), :] = high
        low_r[pl.ds(x * cells_y, cells_y), :] = low

    v_edge, s_edge = first_edges((up2, dn2, up1, dn1), cells_x, cells_y)
    forward_steps(v_r, c_r, v_edge, s_edge, side, finish)
    out_next = copy(next_r, next_h, sems.at[4])
    store_faces(next_r, out_up2, out_dn2, out_up1, out_dn1)
    sent_o[:, 0, 0:capacity] = here
    sent_o[:, 0, capacity:width] = tissue_gather(high_r, low_r, line_r, lane_r, value_r, devices)
    out_soft.wait()
    out_next.wait()


def cable_first_kernel(
    slots, cable, info_i, rows_i, first_own, up2, dn2, up1, dn1, face_up2, face_dn2, face_up1, face_dn1,
    next_o, sent_o, there_o, parent_o, out_up2, out_dn2, out_up1, out_dn1,
):
    devices, _, width = slots.shape
    capacity = width // 2
    info = unpack_info(info_i[...])
    row_info = rows_i[...]
    u = cable[...]
    segments, nodes = u.shape
    first_edge = (up2, dn2, up1, dn1)
    place_x, place_y = up2.shape[0] - 8, up1.shape[0] - 8
    rows = family(u, first_edge, first_own, first_edge, info_i[0:1, 7:8], place_x, place_y)
    flux, parent_tail = cable_flux(u, lane_differences(u), info, *rows)
    before = slots_in(slots[:, 0, 0:capacity], info)
    current = gap_conductance * (node_gather(u, info) - before)
    drawn = node_scatter(current, info, row_info, segments, nodes)
    after = u + time_step * (flux + ionic(u) - drawn)
    next_o[...] = after
    sent_o[:, 0, :] = slots_out(node_gather(after, info), info, row_info, devices, capacity)
    there_o[...] = to_row(slots_in(slots[:, 0, capacity:width], info))
    parent_o[...] = to_row(parent_tail)
    cells_y, cells_x = face_up2.shape[0], face_up1.shape[0]
    for ref, source in (
        (out_up2, face_up2), (out_dn2, face_dn2), (out_up1, face_up1), (out_dn1, face_dn1)
    ):
        count = source.shape[0]
        ref[0:count, :] = source[...]
        ref[count : count + 8, :] = jnp.zeros((8, source.shape[1]), f32)
    store_ends(after, cells_y, cells_x, out_up2, out_dn2, out_up1, out_dn1)


def middle_kernel(
    slots, sent_i, first_slots, info_i, rows_i, first_own, fup2, fdn2, fup1, fdn1, up2, dn2, up1, dn1,
    cable, purkinje_target, there, volt, soft, target,
    next_h, adjoint_h, cable_o, mu_o, sent_o, parent_o, out_up2, out_dn2, out_up1, out_dn1,
    line_r, lane_r, row_r, value_r, high_r, low_r, sum_r, v_r, s_r, t_r, next_r, lam_r, sems,
):
    started = [copy(h, r, sems.at[k]) for k, (h, r) in enumerate(((volt, v_r), (soft, s_r), (target, t_r)))]
    devices, _, capacity = slots.shape
    cells_x, cells_y, cells_z = volt.shape
    side = info_i[0:1, 6:7]
    index = first_slots[:, 0, 0:capacity]
    here = sent_i[:, 0, capacity : 2 * capacity]
    place_slots(index, cells_z, line_r, lane_r, row_r)
    current = jnp.where(index >= 0.0, gap_conductance * (slots[:, 0, :] - here), 0.0)
    tissue_scatter(current, lane_r, row_r, value_r, high_r, low_r, sum_r)
    for each in started:
        each.wait()

    def finish(x, v, s, flux):
        after = v + time_step * (flux + ionic(v) + sum_r[x])
        next_r[x] = after
        wanted = 1.0 - t_r[x].astype(f32) / target_span
        lam = jnp.where(s > 0.0, loss_weight * (after - wanted), 0.0)
        lam_r[x] = lam
        high, low = parts(lam)
        high_r[pl.ds(x * cells_y, cells_y), :] = high
        low_r[pl.ds(x * cells_y, cells_y), :] = low

    first_edge = (fup2, fdn2, fup1, fdn1)
    edge = (up2, dn2, up1, dn1)
    _, s_edge = first_edges(first_edge, cells_x, cells_y)
    forward_steps(v_r, s_r, edge + (0, 0), s_edge, side, finish)
    out_next = copy(next_r, next_h, sems.at[3])
    out_lam = copy(lam_r, adjoint_h, sems.at[4])
    store_faces(lam_r, out_up2, out_dn2, out_up1, out_dn1)
    sent_o[:, 0, 0:capacity] = tissue_gather(high_r, low_r, line_r, lane_r, value_r, devices)

    info = unpack_info(info_i[...])
    row_info = rows_i[...]
    u = cable[...]
    segments, nodes = u.shape
    rows = family(u, edge, first_own, first_edge, info_i[0:1, 7:8], cells_y, cells_x)
    cable_out, parent_tail = cable_flux(u, lane_differences(u), info, *rows)
    drawn = gap_conductance * (node_gather(u, info) - to_column(there[...]))
    drawn = node_scatter(drawn, info, row_info, segments, nodes)
    after = u + time_step * (cable_out + ionic(u) - drawn)
    cable_o[...] = after
    mu = loss_weight * (after - (1.0 - purkinje_target[...].astype(f32) / target_span))
    mu_o[...] = mu
    sent_o[:, 0, capacity : 2 * capacity] = slots_out(
        node_gather(mu, info), info, row_info, devices, capacity
    )
    parent_o[...] = to_row(parent_tail)
    for ref in (out_up2, out_dn2, out_up1, out_dn1):
        count = ref.shape[0]
        ref[count - 8 : count, :] = jnp.zeros((8, cells_z), f32)
    store_ends(mu, cells_y, cells_x, out_up2, out_dn2, out_up1, out_dn1)
    out_next.wait()
    out_lam.wait()


def backward_kernel(last, *refs):
    (slots, sent_i, first_slots, info_i, rows_i, first_own, fup2, fdn2, fup1, fdn1) = refs[:10]
    (vup2, vdn2, vup1, vdn1, up2, dn2, up1, dn1) = refs[10:18]
    (mu_i, cable, parent_old, grad_row, lam_i, volt, soft, grad_i) = refs[18:26]
    outs = refs[26:-13]
    (line_r, lane_r, row_r, value_r, high_r, low_r, sum_r, a_r, v_r, s_r, g_r, next_r, sems) = refs[-13:]
    lam_h, grad_h, mu_o, grad_row_o = outs[:4]
    sources = [(lam_i, a_r), (volt, v_r), (soft, s_r)] + ([(grad_i, g_r)] if last else [])
    started = [copy(h, r, sems.at[k]) for k, (h, r) in enumerate(sources)]
    devices, _, width = slots.shape
    capacity = width // 2
    cells_x, cells_y, cells_z = volt.shape
    side = info_i[0:1, 6:7]
    index = first_slots[:, 0, 0:capacity]
    place_slots(index, cells_z, line_r, lane_r, row_r)
    tissue_here = sent_i[:, 0, 0:capacity]
    cable_here = sent_i[:, 0, capacity:width]
    tissue_there = slots[:, 0, 0:capacity]
    cable_there = slots[:, 0, capacity:width]
    current = jnp.where(index >= 0.0, gap_conductance * (cable_there - tissue_here), 0.0)
    tissue_scatter(current, lane_r, row_r, value_r, high_r, low_r, sum_r)

    first_edge = (fup2, fdn2, fup1, fdn1)
    edge = (up2, dn2, up1, dn1)
    info = unpack_info(info_i[...])
    row_info = rows_i[...]
    mu = mu_i[...]
    u = cable[...]
    segments, nodes = u.shape
    rows = family(mu, edge, first_own, first_edge, info_i[0:1, 7:8], cells_y, cells_x)
    differences = lane_differences(mu)
    cable_out, parent_tail = cable_flux(mu, differences, info, *rows)
    drawn = slots_in(gap_conductance * (cable_here - tissue_there), info)
    drawn = node_scatter(drawn, info, row_info, segments, nodes)
    cable_after = mu + time_step * (cable_out + slope(u) * mu - drawn)
    mu_o[...] = cable_after
    inner = jnp.sum(differences * lane_differences(u), axis=1, keepdims=True)
    head = (mu[:, 0:1] - parent_tail) * (to_column(parent_old[...]) - u[:, 0:1])
    cable_grad = to_row(time_step * (jnp.where(info["parent"] >= 0.0, head, 0.0) - inner))
    grad_row_o[...] = grad_row[...] + cable_grad if last else cable_grad

    for each in started:
        each.wait()

    def finish(x, a, v, flux, product):
        after = a + time_step * (flux + slope(v) * a + sum_r[x])
        next_r[x] = after
        grad = (-0.5 * time_step) * product
        if last:
            g_r[x] = g_r[x] + grad
        else:
            g_r[x] = grad
            high, low = parts(after)
            high_r[pl.ds(x * cells_y, cells_y), :] = high
            low_r[pl.ds(x * cells_y, cells_y), :] = low

    v_first, s_edge = first_edges(first_edge, cells_x, cells_y)
    v_edge = v_first if last else (vup2, vdn2, vup1, vdn1, 0, 0)
    adjoint_steps(a_r, v_r, s_r, edge + (0, 0), v_edge, s_edge, side, finish)
    out_lam = copy(next_r, lam_h, sems.at[4])
    out_grad = copy(g_r, grad_h, sems.at[5])
    if not last:
        sent_o, out_up2, out_dn2, out_up1, out_dn1 = outs[4:]
        store_faces(next_r, out_up2, out_dn2, out_up1, out_dn1)
        sent_o[:, 0, 0:capacity] = tissue_gather(high_r, low_r, line_r, lane_r, value_r, devices)
        sent_o[:, 0, capacity:width] = slots_out(
            node_gather(cable_after, info), info, row_info, devices, capacity
        )
        for ref in (out_up2, out_dn2, out_up1, out_dn1):
            count = ref.shape[0]
            ref[count - 8 : count, :] = jnp.zeros((8, cells_z), f32)
        store_ends(cable_after, cells_y, cells_x, out_up2, out_dn2, out_up1, out_dn1)
    out_lam.wait()
    out_grad.wait()


def shifted(block, distance):
    axes = ("gx", "gy")
    devices = range(lax.axis_size(axes))
    return lax.ppermute(block, axes, [(i - distance, i) for i in devices if i - distance in devices])


def neighbours(up2, dn2, up1, dn1):
    return shifted(up2, 2), shifted(dn2, -2), shifted(up1, 1), shifted(dn1, -1)


def swap_slots(slots):
    return lax.all_to_all(slots, ("gx", "gy"), split_axis=0, concat_axis=0, tiled=True)


def body(
    initial_voltage,
    conductivity,
    tissue_mask,
    target_step,
    initial_purkinje,
    purkinje_conductivity,
    segment_parent,
    purkinje_target,
    junction_voxel,
    junction_node,
):
    shape = initial_voltage.shape
    cells_x, cells_y, cells_z = shape
    segments, nodes = initial_purkinje.shape
    grid_x, grid_y = lax.axis_size("gx"), lax.axis_size("gy")
    devices = grid_x * grid_y
    per_device = junction_voxel.shape[0]
    capacity = max(2, 2 * per_device // devices)
    slots = devices * capacity
    plane = cells_y * grid_y * cells_z
    side = lax.axis_index("gy")
    first = lax.axis_index(("gx", "gy")) * segments
    scal = jnp.stack([side, first]).astype(i32)
    one = sds((1, segments))
    cable_shape = sds((segments, nodes))
    tissue_shape = sds(shape)
    double = sds((devices, 1, 2 * capacity))
    faces = [sds((n, cells_z)) for n in (cells_y, cells_y, cells_x, cells_x)]
    payload = [sds((n + 8, cells_z)) for n in (cells_y, cells_y, cells_x, cells_x)]
    payload0 = [sds((2 * n + 8, cells_z)) for n in (cells_y, cells_y, cells_x, cells_x)]
    whole = pltpu.VMEM(shape, f32)
    whole_int = pltpu.VMEM(shape, i32)
    work = field_scratch(slots, shape)

    sent0, info, rows, *out0 = call(
        functools.partial(setup_kernel, plane, cells_y, cells_z, cells_x, grid_y),
        "setup",
        near(double, sds((segments, 128)), sds((8, segments)), *payload0),
        near(
            junction_voxel.reshape(1, -1),
            junction_node.reshape(1, -1),
            segment_parent.reshape(1, -1),
            purkinje_conductivity.reshape(1, -1),
            initial_purkinje,
        )
        + far(initial_voltage, conductivity, tissue_mask),
        [
            pltpu.VMEM((2, cells_y, cells_z), f32),
            pltpu.VMEM((2, cells_y, cells_z), f32),
            pltpu.VMEM((2, cells_y, cells_z), i32),
            pltpu.VMEM((2, cells_x, 8, cells_z), f32),
            pltpu.VMEM((2, cells_x, 8, cells_z), f32),
            pltpu.VMEM((2, cells_x, 8, cells_z), i32),
            DMA((12,)),
        ],
        scal,
    )
    arrived0 = swap_slots(sent0)
    edge0 = neighbours(*out0)
    own0 = out0[3]

    voltage1, soft, sent1, *faces1 = call(
        tissue_first_kernel,
        "tissue_first",
        far(tissue_shape, tissue_shape) + near(double, *faces),
        near(arrived0, info, *edge0) + far(initial_voltage, conductivity, tissue_mask),
        work + [whole, whole, whole_int, whole, DMA((5,))],
    )
    arrived1 = swap_slots(sent1)
    cable1, sent2, there1, parent0, *out1 = call(
        cable_first_kernel,
        "cable_first",
        near(cable_shape, sds((devices, 1, capacity)), one, one, *payload),
        near(arrived1, initial_purkinje, info, rows, own0, *edge0, *faces1),
    )
    arrived2 = swap_slots(sent2)
    edge1 = neighbours(*out1)
    voltage2, lam2, cable2, mu2, sent3, parent1, *out2 = call(
        middle_kernel,
        "middle",
        far(tissue_shape, tissue_shape) + near(cable_shape, cable_shape, double, one, *payload),
        near(arrived2, sent1, arrived0, info, rows, own0, *edge0, *edge1, cable1, purkinje_target, there1)
        + far(voltage1, soft, target_step),
        work + [whole, whole, whole_int, whole, whole, DMA((5,))],
    )

    def backward(last, sent, out, lam, volt, volt_edge, mu, old, parent_old, grads):
        arrived = swap_slots(sent)
        edge = neighbours(*out)
        outs = far(tissue_shape, tissue_shape) + near(cable_shape, one)
        if not last:
            outs += near(double, *payload)
        return call(
            functools.partial(backward_kernel, last),
            "backward",
            outs,
            near(arrived, sent, arrived0, info, rows, own0, *edge0, *volt_edge, *edge)
            + near(mu, old, parent_old, grads[1])
            + far(lam, volt, soft, grads[0]),
            work + [whole, whole, whole, whole, whole, DMA((6,))],
        )

    lam1, grad, mu1, grad_row, sent4, *out3 = backward(
        False, sent3, out2, lam2, voltage1, edge1, mu2, cable1, parent1, (lam2, parent1)
    )
    lam0, grad, mu0, grad_row = backward(
        True, sent4, out3, lam1, initial_voltage, edge1, mu1, initial_purkinje, parent0, (grad, grad_row)
    )
    return (voltage2, cable2, grad, grad_row.reshape(-1), lam0, mu0)


def solution(mesh):
    tissue = P(("groups", "gx"), "gy", None)
    cable = P(("groups", "gx", "gy"), None)
    flat = P(("groups", "gx", "gy"))
    in_specs = (tissue, tissue, tissue, tissue, cable, flat, flat, cable, flat, flat)
    out_specs = (tissue, cable, tissue, flat, tissue, cable)
    return jax.shard_map(body, mesh=mesh, in_specs=in_specs, out_specs=out_specs, check_vma=False)
```

```python
import functools

import jax
import jax.numpy as jnp
from jax import lax
from jax.experimental import pallas as pl
from jax.experimental.pallas import tpu as pltpu
from jax.sharding import PartitionSpec as P


time_step = 0.05
gap_conductance = 4.0
ion_rate = 8.0
threshold = 0.15
loss_weight = 10.0
target_span = 8.0

INTERPRET = False
f32 = jnp.float32
bf16 = jnp.bfloat16
i32 = jnp.int32
FAR = -1.0e7
LIMIT = 60 << 20


def sds(shape, dtype=f32):
    return jax.ShapeDtypeStruct(shape, dtype)


DMA = pltpu.SemaphoreType.DMA


def call(kernel, outs, arrays, scratch=(), scalars=None, flops=20_000_000):
    def spec(inside):
        return pl.BlockSpec(memory_space=pltpu.VMEM if inside else pl.ANY)

    specs = [pl.BlockSpec(memory_space=pltpu.SMEM)] if scalars is not None else []
    specs += [spec(inside) for _, inside in arrays]
    args = ([scalars] if scalars is not None else []) + [a for a, _ in arrays]
    return pl.pallas_call(
        kernel,
        out_shape=[o for o, _ in outs],
        in_specs=specs,
        out_specs=[spec(inside) for _, inside in outs],
        scratch_shapes=list(scratch),
        compiler_params=pltpu.CompilerParams(vmem_limit_bytes=LIMIT),
        cost_estimate=pl.CostEstimate(flops=flops, transcendentals=0, bytes_accessed=4_000_000),
        interpret=INTERPRET,
    )(*args)


def near(*arrays):
    return [(a, True) for a in arrays]


def far(*arrays):
    return [(a, False) for a in arrays]


def copy(source, target, sem):
    started = pltpu.make_async_copy(source, target, sem)
    started.start()
    return started


def ionic(values):
    return ion_rate * values * (values - threshold) * (1.0 - values)


def slope(values):
    return ion_rate * (-3.0 * values * values + 2.0 * (1.0 + threshold) * values - threshold)


def iota(shape, dim):
    return lax.broadcasted_iota(i32, shape, dim)


def parts(values):
    high = values.astype(bf16)
    return high, (values - high.astype(f32)).astype(bf16)


def parts_dot(chooser, pieces):
    total = None
    for piece in pieces:
        term = jnp.dot(chooser, piece, preferred_element_type=f32)
        total = term if total is None else total + term
    return total


def exact_parts(values):
    high = values.astype(bf16)
    rest = values - high.astype(f32)
    middle = rest.astype(bf16)
    return high, middle, (rest - middle.astype(f32)).astype(bf16)


def one_hot(test):
    return jnp.where(test, 1.0, 0.0).astype(bf16)


def to_row(column):
    count = column.shape[0]
    eye = iota((128, 128), 0) == iota((128, 128), 1)
    rows = []
    for first in range(0, count, 128):
        spread = jnp.broadcast_to(column[first : first + 128], (128, 128))
        rows.append(jnp.sum(jnp.where(eye, spread, 0.0), axis=0, keepdims=True))
    return jnp.concatenate(rows, axis=1)


def to_column(row):
    count = row.shape[1]
    eye = iota((128, 128), 0) == iota((128, 128), 1)
    columns = []
    for first in range(0, count, 128):
        spread = jnp.broadcast_to(row[:, first : first + 128], (128, 128))
        columns.append(jnp.sum(jnp.where(eye, spread, 0.0), axis=1, keepdims=True))
    return jnp.concatenate(columns, axis=0)


def put_line(ref, place, row):
    width = ref.shape[1]
    for k in range(row.shape[1] // width):
        ref[place + k : place + k + 1, :] = row[:, k * width : (k + 1) * width]


def get_line(ref, place, length):
    width = ref.shape[1]
    return jnp.concatenate([ref[place + k : place + k + 1, :] for k in range(length // width)], axis=1)


def spread_slots(table, ref):
    devices, capacity = table.shape
    for rank in range(capacity):
        ref[rank * devices : (rank + 1) * devices, :] = jnp.broadcast_to(
            table[:, rank : rank + 1], (devices, 128)
        )


def place_slots(index, cells_z, line_ref, lane_ref, row_ref):
    whole = index.astype(i32)
    line = whole // cells_z
    lane = whole - line * cells_z
    line = jnp.where(whole < 0, -1, line)
    spread_slots(line.astype(f32), line_ref)
    spread_slots(lane.astype(f32), lane_ref)
    slots = line_ref.shape[0]
    eye = iota((128, 128), 0) == iota((128, 128), 1)
    for first in range(0, slots, 128):
        block = jnp.where(eye, line_ref[first : first + 128, :], 0.0)
        row_ref[:, first : first + 128] = jnp.sum(block, axis=0, keepdims=True)


def split_field(values_ref, high_ref, low_ref):
    cells_x, cells_y, _ = values_ref.shape

    def step(x, _):
        high, low = parts(values_ref[x])
        high_ref[pl.ds(x * cells_y, cells_y), :] = high
        low_ref[pl.ds(x * cells_y, cells_y), :] = low
        return 0

    lax.fori_loop(0, cells_x, step, 0)


def tissue_gather(high_ref, low_ref, line_ref, lane_ref, value_ref, devices):
    slots = line_ref.shape[0]
    lines, width = high_ref.shape
    block = 256
    along = iota((block, 128), 1).astype(f32)

    def step(b, _):
        where = pl.ds(b * block, block)
        line = line_ref[where, :]
        lane = lane_ref[where, :]
        chooser = jnp.concatenate(
            [one_hot(line == along + float(first)) for first in range(0, lines, 128)], axis=1
        )
        taken = parts_dot(chooser, (high_ref[...], low_ref[...]))
        kept = jnp.zeros((block, 128), f32)
        for first in range(0, width, 128):
            kept = kept + jnp.where(lane == along + float(first), taken[:, first : first + 128], 0.0)
        value_ref[where, :] = jnp.broadcast_to(jnp.sum(kept, axis=1, keepdims=True), (block, 128))
        return 0

    lax.fori_loop(0, slots // block, step, 0)
    capacity = slots // devices
    table = jnp.zeros((devices, capacity), f32)
    which = iota((devices, capacity), 1)
    for rank in range(capacity):
        table = jnp.where(
            which == rank, value_ref[rank * devices : (rank + 1) * devices, 0:capacity], table
        )
    return table


def tissue_scatter(current, lane_ref, row_ref, value_ref, high_ref, low_ref, sum_ref):
    slots = lane_ref.shape[0]
    cells_x, cells_y, width = sum_ref.shape
    spread_slots(current, value_ref)
    along = iota((128, 128), 1).astype(f32)

    def build(b, _):
        where = pl.ds(b * 128, 128)
        lane = lane_ref[where, :]
        high, low = parts(value_ref[where, :])
        for first in range(0, width, 128):
            hit = lane == along + float(first)
            high_ref[where, first : first + 128] = jnp.where(hit, high.astype(f32), 0.0).astype(bf16)
            low_ref[where, first : first + 128] = jnp.where(hit, low.astype(f32), 0.0).astype(bf16)
        return 0

    lax.fori_loop(0, slots // 128, build, 0)
    slabs = 256 // cells_y
    down = iota((slabs * cells_y, slots), 0).astype(f32)

    def step(b, _):
        base = (b * slabs * cells_y).astype(f32)
        chooser = one_hot(down == row_ref[...] - base)
        added = parts_dot(chooser, (high_ref[...], low_ref[...]))
        sum_ref[pl.ds(b * slabs, slabs)] = added.reshape(slabs, cells_y, width)
        return 0

    lax.fori_loop(0, cells_x // slabs, step, 0)


def field_scratch(slots, shape):
    lines = shape[0] * shape[1]
    assert slots == lines
    wide = pltpu.VMEM((lines, shape[2]), bf16)
    return [
        pltpu.VMEM((slots, 128), f32),
        pltpu.VMEM((slots, 128), f32),
        pltpu.VMEM((1, slots), f32),
        pltpu.VMEM((slots, 128), f32),
        wide,
        wide,
        pltpu.VMEM(shape, f32),
    ]


def shift_up_y(slab, high):
    rolled = pltpu.roll(slab, slab.shape[0] - 1, 0)
    return jnp.where(iota(slab.shape, 0) == slab.shape[0] - 1, high, rolled)


def shift_down_y(slab, low):
    return jnp.where(iota(slab.shape, 0) == 0, low, pltpu.roll(slab, 1, 0))


def shift_up_z(slab):
    return pltpu.roll(slab, slab.shape[1] - 1, 1)


def shift_down_z(slab):
    return pltpu.roll(slab, 1, 1)


def face(a, b):
    return jnp.where(jnp.minimum(a, b) > 0.0, 0.5 * (a + b), 0.0)


def each_slab(count, step, first_carry):
    carry = lax.fori_loop(0, count - 1, lambda x, c: step(x, c, False), first_carry)
    return step(count - 1, carry, True)


def y_lines(low_ref, high_ref, place, x, side):
    low = jnp.where(side == 1.0, low_ref[pl.ds(place + x, 1), :], 0.0)
    high = jnp.where(side == 0.0, high_ref[pl.ds(place + x, 1), :], 0.0)
    return low, high


def forward_steps(v_ref, s_ref, v_edge, s_edge, side, finish):
    cells_x, cells_y, cells_z = v_ref.shape
    last_lane = iota((cells_y, cells_z), 1) == cells_z - 1
    vxl, vxh, vyl, vyh, vx, vy = v_edge
    sxl, sxh, syl, syh, sx, sy = s_edge

    def step(x, carry, last):
        v = v_ref[x]
        s = s_ref[x]
        if last:
            vn, sn = vxh[vx : vx + cells_y, :], sxh[sx : sx + cells_y, :]
        else:
            vn, sn = v_ref[x + 1], s_ref[x + 1]
        vl, vh = y_lines(vyl, vyh, vy, x, side)
        sl, sh = y_lines(syl, syh, sy, x, side)
        fx = face(s, sn) * (vn - v)
        fy = face(s, shift_up_y(s, sh)) * (shift_up_y(v, vh) - v)
        fyl = face(s[0:1], sl) * (v[0:1] - vl)
        fz = jnp.where(last_lane, 0.0, face(s, shift_up_z(s)) * (shift_up_z(v) - v))
        finish(x, v, s, fx - carry + fy - shift_down_y(fy, fyl) + fz - shift_down_z(fz))
        return fx

    low_v, low_s = vxl[vx : vx + cells_y, :], sxl[sx : sx + cells_y, :]
    each_slab(cells_x, step, face(s_ref[0], low_s) * (v_ref[0] - low_v))


def adjoint_steps(a_ref, v_ref, s_ref, a_edge, v_edge, s_edge, side, finish):
    cells_x, cells_y, cells_z = v_ref.shape
    last_lane = iota((cells_y, cells_z), 1) == cells_z - 1
    axl, axh, ayl, ayh, ax, ay = a_edge
    vxl, vxh, vyl, vyh, vx, vy = v_edge
    sxl, sxh, syl, syh, sx, sy = s_edge

    def pair(s, sn, d, e):
        both = jnp.minimum(s, sn) > 0.0
        d = jnp.where(both, d, 0.0)
        return (0.5 * (s + sn)) * d, d * e

    def step(x, carry, last):
        flux_before, product_before = carry
        a = a_ref[x]
        v = v_ref[x]
        s = s_ref[x]
        if last:
            an = axh[ax : ax + cells_y, :]
            vn = vxh[vx : vx + cells_y, :]
            sn = sxh[sx : sx + cells_y, :]
        else:
            an, vn, sn = a_ref[x + 1], v_ref[x + 1], s_ref[x + 1]
        al, ah = y_lines(ayl, ayh, ay, x, side)
        vl, vh = y_lines(vyl, vyh, vy, x, side)
        sl, sh = y_lines(syl, syh, sy, x, side)
        fx, px = pair(s, sn, an - a, vn - v)
        fy, py = pair(s, shift_up_y(s, sh), shift_up_y(a, ah) - a, shift_up_y(v, vh) - v)
        fyl, pyl = pair(s[0:1], sl, a[0:1] - al, v[0:1] - vl)
        dz = jnp.where(last_lane, 0.0, shift_up_z(a) - a)
        fz, pz = pair(s, shift_up_z(s), dz, shift_up_z(v) - v)
        flux = fx - flux_before + fy - shift_down_y(fy, fyl) + fz - shift_down_z(fz)
        product = px + product_before + py + shift_down_y(py, pyl) + pz + shift_down_z(pz)
        finish(x, a, v, flux, product)
        return fx, px

    low = [ref[at : at + cells_y, :] for ref, at in ((axl, ax), (vxl, vx), (sxl, sx))]
    each_slab(cells_x, step, pair(s_ref[0], low[2], a_ref[0] - low[0], v_ref[0] - low[1]))


def store_faces(values_ref, up2, dn2, up1, dn1):
    cells_x, cells_y, _ = values_ref.shape
    dn2[0:cells_y, :] = values_ref[0]
    up2[0:cells_y, :] = values_ref[cells_x - 1]
    for x in range(cells_x):
        dn1[x : x + 1, :] = values_ref[x, 0:1, :]
        up1[x : x + 1, :] = values_ref[x, cells_y - 1 : cells_y, :]


def store_ends(values, place_x, place_y, up2, dn2, up1, dn1):
    nodes = values.shape[1]
    tail = to_row(values[:, nodes - 1 : nodes])
    head = to_row(values[:, 0:1])
    put_line(up2, place_x, tail)
    put_line(up1, place_y, tail)
    put_line(dn2, place_x, head)
    put_line(dn1, place_y, head)


def unpack_info(info):
    names = ("device", "rank", "segment", "node", "sigma", "parent")
    return {name: info[:, k : k + 1] for k, name in enumerate(names)}


def slots_out(column, info, row_info, devices, capacity, split=parts):
    put = one_hot(iota((devices, column.shape[0]), 0).astype(f32) == row_info[0:1, :])
    chosen = info["rank"] == iota((1, capacity), 1).astype(f32)
    pieces = [jnp.where(chosen, piece.astype(f32), 0.0).astype(bf16) for piece in split(column)]
    return parts_dot(put, pieces)


def slots_in(slots, info):
    devices, capacity = slots.shape
    pick = one_hot(info["device"] == iota((1, devices), 1).astype(f32))
    taken = parts_dot(pick, parts(slots))
    chosen = info["rank"] == iota((1, capacity), 1).astype(f32)
    return jnp.sum(jnp.where(chosen, taken, 0.0), axis=1, keepdims=True)


def node_gather(values, info):
    segments, nodes = values.shape
    pick = one_hot(info["segment"] == iota((1, segments), 1).astype(f32))
    taken = parts_dot(pick, parts(values))
    chosen = info["node"] == iota((1, nodes), 1).astype(f32)
    return jnp.sum(jnp.where(chosen, taken, 0.0), axis=1, keepdims=True)


def node_scatter(column, info, row_info, segments, nodes):
    put = one_hot(iota((segments, 1), 0).astype(f32) == row_info[1:2, :])
    chosen = info["node"] == iota((1, nodes), 1).astype(f32)
    pieces = [jnp.where(chosen, piece.astype(f32), 0.0).astype(bf16) for piece in parts(column)]
    return parts_dot(put, pieces)


def lane_differences(values):
    nodes = values.shape[1]
    inside = iota(values.shape, 1) < nodes - 1
    return jnp.where(inside, pltpu.roll(values, nodes - 1, 1) - values, 0.0)


def window_pick(info, window):
    lines = [window[:, first : first + 128] for first in range(0, window.shape[1], 128)]
    lines.append(jnp.zeros((-len(lines) % 16, 128), f32))
    place = info["parent"].astype(i32)
    pick = one_hot(place >> 7 == iota((1, 16), 1))
    taken = parts_dot(pick, exact_parts(jnp.concatenate(lines, axis=0)))
    return jnp.sum(jnp.where(place & 127 == iota((1, 128), 1), taken, 0.0), axis=1, keepdims=True)


def cable_flux(values, differences, info, tails, heads, child_sigma, child_parent):
    segments, nodes = values.shape
    edge = info["sigma"] * differences
    result = edge - pltpu.roll(edge, 1, 1)
    parent_tail = window_pick(info, tails)
    own_head = values[:, 0:1]
    own_tail = values[:, nodes - 1 : nodes]
    head_flux = jnp.where(info["parent"] >= 0.0, info["sigma"] * (parent_tail - own_head), 0.0)
    mine = child_parent == iota((segments, 1), 0).astype(f32)
    inflow = jnp.sum(
        jnp.where(mine, child_sigma * (heads - own_tail), 0.0), axis=1, keepdims=True
    )
    lane = iota(values.shape, 1)
    result = result + jnp.where(lane == 0, head_flux, 0.0)
    result = result + jnp.where(lane == nodes - 1, inflow, 0.0)
    return result, parent_tail


def join(rows):
    return jnp.concatenate(rows, axis=1)


def family(values, edge, first_own, first_edge, first_device, place_x, place_y):
    segments, nodes = values.shape
    up2, dn2, up1, dn1 = edge
    _, first_dn2, _, first_dn1 = first_edge
    tail = to_row(values[:, nodes - 1 : nodes])
    head = to_row(values[:, 0:1])
    lines = segments // up2.shape[1]
    fx = first_dn2.shape[0] - 8
    fy = first_dn1.shape[0] - 8
    tails = join([get_line(up2, place_x, segments), get_line(up1, place_y, segments), tail])
    heads = join([head, get_line(dn1, place_y, segments), get_line(dn2, place_x, segments)])
    both = []
    for k in (1, 2):
        both.append(
            join(
                [
                    get_line(first_own, fy + k * lines, segments),
                    get_line(first_dn1, fy + k * lines, segments),
                    get_line(first_dn2, fx + k * lines, segments),
                ]
            )
        )
    return tails, heads, both[0], both[1] - first_device


def setup_kernel(
    plane, cells_y, cells_z, cells_x, grid_y,
    scal, voxel, node, parent, sigma, cable, volt, cond, mask,
    slots_o, info_o, rows_o, up2, dn2, up1, dn1,
    face_v, face_c, face_m, row_v, row_c, row_m, sems,
):
    high = cells_y - 8
    started = []
    for k, (whole, faces, rows) in enumerate(
        ((volt, face_v, row_v), (cond, face_c, row_c), (mask, face_m, row_m))
    ):
        started.append(copy(whole.at[0], faces.at[0], sems.at[4 * k]))
        started.append(copy(whole.at[cells_x - 1], faces.at[1], sems.at[4 * k + 1]))
        started.append(copy(whole.at[:, pl.ds(0, 8), :], rows.at[0], sems.at[4 * k + 2]))
        started.append(copy(whole.at[:, pl.ds(high, 8), :], rows.at[1], sems.at[4 * k + 3]))
    segments, nodes = cable.shape
    count = voxel.shape[1]
    devices, _, width = slots_o.shape
    capacity = width // 2
    first = scal[1]
    vox = voxel[...]
    coord_x = vox // plane
    inside = vox - coord_x * plane
    coord_y = inside // cells_z
    coord_z = inside - coord_y * cells_z
    block_x = coord_x // cells_x
    block_y = coord_y // cells_y
    device = (block_x * grid_y + block_y).astype(f32)
    local = ((coord_x - block_x * cells_x) * cells_y + coord_y - block_y * cells_y) * cells_z + coord_z
    spot = node[...] - first * nodes
    segment = spot // nodes
    lane = (spot - segment * nodes).astype(f32)
    segment = segment.astype(f32)
    own_parent = parent[...]
    relative = jnp.where(own_parent >= 0, (own_parent - first + 2 * segments).astype(f32), FAR)
    device_column = to_column(device)
    earlier = iota((count, count), 1) < iota((count, count), 0)
    same = (device_column == device) & earlier
    rank = jnp.sum(jnp.where(same, 1.0, 0.0), axis=1, keepdims=True)
    columns = [
        device_column,
        rank,
        to_column(segment),
        to_column(lane),
        to_column(sigma[...]),
        to_column(relative),
        scal[0].astype(f32),
        first.astype(f32),
    ]
    spread = jnp.zeros((segments, 128), f32)
    where = iota((segments, 128), 1)
    for k, column in enumerate(columns):
        spread = jnp.where(where == k, column, spread)
    info_o[...] = spread
    rows_o[...] = jnp.zeros(rows_o.shape, f32)
    rows_o[0:1, :] = device
    rows_o[1:2, :] = segment
    info = unpack_info(spread)
    row_info = rows_o[...]
    value = node_gather(cable[...], info)
    index = slots_out(
        to_column((local + 1).astype(f32)), info, row_info, devices, capacity, exact_parts
    ) - 1.0
    slots_o[:, 0, 0:capacity] = index
    slots_o[:, 0, capacity:width] = slots_out(value, info, row_info, devices, capacity)
    place_x, place_y = 2 * cells_y, 2 * cells_x
    for ref, place in ((up2, place_x), (dn2, place_x), (up1, place_y), (dn1, place_y)):
        ref[place : place + 8, :] = jnp.zeros((8, cells_z), f32)
    store_ends(cable[...], place_x, place_y, up2, dn2, up1, dn1)
    lines = segments // cells_z
    plain_parent = jnp.where(own_parent >= 0, own_parent.astype(f32), FAR)
    for ref, place in ((dn2, place_x), (dn1, place_y)):
        put_line(ref, place + lines, sigma[...])
        put_line(ref, place + 2 * lines, plain_parent)
    for each in started:
        each.wait()
    for k, ref in ((0, dn2), (1, up2)):
        ref[0:cells_y, :] = face_v[k]
        ref[cells_y : 2 * cells_y, :] = face_c[k] * face_m[k].astype(f32)
    for k, at, ref in ((0, 0, dn1), (1, 7, up1)):
        for x in range(cells_x):
            ref[x : x + 1, :] = row_v[k, x, at : at + 1, :]
            ref[cells_x + x : cells_x + x + 1, :] = (
                row_c[k, x, at : at + 1, :] * row_m[k, x, at : at + 1, :].astype(f32)
            )


def first_edges(edge, cells_x, cells_y):
    up2, dn2, up1, dn1 = edge
    return (up2, dn2, up1, dn1, 0, 0), (up2, dn2, up1, dn1, cells_y, cells_x)


def tissue_first_kernel(
    slots, info_i, up2, dn2, up1, dn1, volt, cond, mask,
    next_h, soft_h, sent_o, out_up2, out_dn2, out_up1, out_dn1,
    line_r, lane_r, row_r, value_r, high_r, low_r, sum_r, v_r, c_r, m_r, next_r, sems,
):
    started = [copy(h, r, sems.at[k]) for k, (h, r) in enumerate(((volt, v_r), (cond, c_r), (mask, m_r)))]
    devices, _, width = slots.shape
    capacity = width // 2
    cells_x, cells_y, cells_z = volt.shape
    side = info_i[0:1, 6:7]
    index = slots[:, 0, 0:capacity]
    there = slots[:, 0, capacity:width]
    place_slots(index, cells_z, line_r, lane_r, row_r)
    for each in started:
        each.wait()

    def prepare(x, _):
        c_r[x] = c_r[x] * m_r[x].astype(f32)
        return 0

    lax.fori_loop(0, cells_x, prepare, 0)
    out_soft = copy(c_r, soft_h, sems.at[3])
    split_field(v_r, high_r, low_r)
    here = tissue_gather(high_r, low_r, line_r, lane_r, value_r, devices)
    current = jnp.where(index >= 0.0, gap_conductance * (there - here), 0.0)
    tissue_scatter(current, lane_r, row_r, value_r, high_r, low_r, sum_r)

    def finish(x, v, s, flux):
        after = v + time_step * (flux + ionic(v) + sum_r[x])
        next_r[x] = after
        high, low = parts(after)
        high_r[pl.ds(x * cells_y, cells_y), :] = high
        low_r[pl.ds(x * cells_y, cells_y), :] = low

    v_edge, s_edge = first_edges((up2, dn2, up1, dn1), cells_x, cells_y)
    forward_steps(v_r, c_r, v_edge, s_edge, side, finish)
    store_faces(next_r, out_up2, out_dn2, out_up1, out_dn1)
    out_next = copy(next_r, next_h, sems.at[4])
    sent_o[:, 0, 0:capacity] = here
    sent_o[:, 0, capacity:width] = tissue_gather(high_r, low_r, line_r, lane_r, value_r, devices)
    out_soft.wait()
    out_next.wait()


def cable_first_kernel(
    slots, cable, info_i, rows_i, first_own, up2, dn2, up1, dn1, face_up2, face_dn2, face_up1, face_dn1,
    next_o, sent_o, there_o, parent_o, out_up2, out_dn2, out_up1, out_dn1,
):
    devices, _, width = slots.shape
    capacity = width // 2
    info = unpack_info(info_i[...])
    row_info = rows_i[...]
    u = cable[...]
    segments, nodes = u.shape
    first_edge = (up2, dn2, up1, dn1)
    place_x, place_y = up2.shape[0] - 8, up1.shape[0] - 8
    rows = family(u, first_edge, first_own, first_edge, info_i[0:1, 7:8], place_x, place_y)
    flux, parent_tail = cable_flux(u, lane_differences(u), info, *rows)
    before = slots_in(slots[:, 0, 0:capacity], info)
    current = gap_conductance * (node_gather(u, info) - before)
    drawn = node_scatter(current, info, row_info, segments, nodes)
    after = u + time_step * (flux + ionic(u) - drawn)
    next_o[...] = after
    sent_o[:, 0, :] = slots_out(node_gather(after, info), info, row_info, devices, capacity)
    there_o[...] = to_row(slots_in(slots[:, 0, capacity:width], info))
    parent_o[...] = to_row(parent_tail)
    cells_y, cells_x = face_up2.shape[0], face_up1.shape[0]
    for ref, source in (
        (out_up2, face_up2), (out_dn2, face_dn2), (out_up1, face_up1), (out_dn1, face_dn1)
    ):
        count = source.shape[0]
        ref[0:count, :] = source[...]
        ref[count : count + 8, :] = jnp.zeros((8, source.shape[1]), f32)
    store_ends(after, cells_y, cells_x, out_up2, out_dn2, out_up1, out_dn1)


def middle_kernel(
    slots, sent_i, first_slots, info_i, rows_i, first_own, fup2, fdn2, fup1, fdn1, up2, dn2, up1, dn1,
    cable, purkinje_target, there, volt, soft, target,
    next_h, adjoint_h, cable_o, mu_o, sent_o, parent_o, out_up2, out_dn2, out_up1, out_dn1,
    line_r, lane_r, row_r, value_r, high_r, low_r, sum_r, v_r, s_r, t_r, next_r, lam_r, sems,
):
    started = [copy(h, r, sems.at[k]) for k, (h, r) in enumerate(((volt, v_r), (soft, s_r), (target, t_r)))]
    devices, _, capacity = slots.shape
    cells_x, cells_y, cells_z = volt.shape
    side = info_i[0:1, 6:7]
    index = first_slots[:, 0, 0:capacity]
    here = sent_i[:, 0, capacity : 2 * capacity]
    place_slots(index, cells_z, line_r, lane_r, row_r)
    current = jnp.where(index >= 0.0, gap_conductance * (slots[:, 0, :] - here), 0.0)
    tissue_scatter(current, lane_r, row_r, value_r, high_r, low_r, sum_r)
    for each in started:
        each.wait()

    def finish(x, v, s, flux):
        after = v + time_step * (flux + ionic(v) + sum_r[x])
        next_r[x] = after
        wanted = 1.0 - t_r[x].astype(f32) / target_span
        lam = jnp.where(s > 0.0, loss_weight * (after - wanted), 0.0)
        lam_r[x] = lam
        high, low = parts(lam)
        high_r[pl.ds(x * cells_y, cells_y), :] = high
        low_r[pl.ds(x * cells_y, cells_y), :] = low

    first_edge = (fup2, fdn2, fup1, fdn1)
    edge = (up2, dn2, up1, dn1)
    _, s_edge = first_edges(first_edge, cells_x, cells_y)
    forward_steps(v_r, s_r, edge + (0, 0), s_edge, side, finish)
    out_next = copy(next_r, next_h, sems.at[3])
    out_lam = copy(lam_r, adjoint_h, sems.at[4])
    store_faces(lam_r, out_up2, out_dn2, out_up1, out_dn1)
    sent_o[:, 0, 0:capacity] = tissue_gather(high_r, low_r, line_r, lane_r, value_r, devices)

    info = unpack_info(info_i[...])
    row_info = rows_i[...]
    u = cable[...]
    segments, nodes = u.shape
    rows = family(u, edge, first_own, first_edge, info_i[0:1, 7:8], cells_y, cells_x)
    cable_out, parent_tail = cable_flux(u, lane_differences(u), info, *rows)
    drawn = gap_conductance * (node_gather(u, info) - to_column(there[...]))
    drawn = node_scatter(drawn, info, row_info, segments, nodes)
    after = u + time_step * (cable_out + ionic(u) - drawn)
    cable_o[...] = after
    mu = loss_weight * (after - (1.0 - purkinje_target[...].astype(f32) / target_span))
    mu_o[...] = mu
    sent_o[:, 0, capacity : 2 * capacity] = slots_out(
        node_gather(mu, info), info, row_info, devices, capacity
    )
    parent_o[...] = to_row(parent_tail)
    for ref in (out_up2, out_dn2, out_up1, out_dn1):
        count = ref.shape[0]
        ref[count - 8 : count, :] = jnp.zeros((8, cells_z), f32)
    store_ends(mu, cells_y, cells_x, out_up2, out_dn2, out_up1, out_dn1)
    out_next.wait()
    out_lam.wait()


def backward_kernel(last, *refs):
    (slots, sent_i, first_slots, info_i, rows_i, first_own, fup2, fdn2, fup1, fdn1) = refs[:10]
    (vup2, vdn2, vup1, vdn1, up2, dn2, up1, dn1) = refs[10:18]
    (mu_i, cable, parent_old, grad_row, lam_i, volt, soft, grad_i) = refs[18:26]
    outs = refs[26:-13]
    (line_r, lane_r, row_r, value_r, high_r, low_r, sum_r, a_r, v_r, s_r, g_r, next_r, sems) = refs[-13:]
    lam_h, grad_h, mu_o, grad_row_o = outs[:4]
    sources = [(lam_i, a_r), (volt, v_r), (soft, s_r)] + ([(grad_i, g_r)] if last else [])
    started = [copy(h, r, sems.at[k]) for k, (h, r) in enumerate(sources)]
    devices, _, width = slots.shape
    capacity = width // 2
    cells_x, cells_y, cells_z = volt.shape
    side = info_i[0:1, 6:7]
    index = first_slots[:, 0, 0:capacity]
    place_slots(index, cells_z, line_r, lane_r, row_r)
    tissue_here = sent_i[:, 0, 0:capacity]
    cable_here = sent_i[:, 0, capacity:width]
    tissue_there = slots[:, 0, 0:capacity]
    cable_there = slots[:, 0, capacity:width]
    current = jnp.where(index >= 0.0, gap_conductance * (cable_there - tissue_here), 0.0)
    tissue_scatter(current, lane_r, row_r, value_r, high_r, low_r, sum_r)

    first_edge = (fup2, fdn2, fup1, fdn1)
    edge = (up2, dn2, up1, dn1)
    info = unpack_info(info_i[...])
    row_info = rows_i[...]
    mu = mu_i[...]
    u = cable[...]
    segments, nodes = u.shape
    rows = family(mu, edge, first_own, first_edge, info_i[0:1, 7:8], cells_y, cells_x)
    differences = lane_differences(mu)
    cable_out, parent_tail = cable_flux(mu, differences, info, *rows)
    drawn = slots_in(gap_conductance * (cable_here - tissue_there), info)
    drawn = node_scatter(drawn, info, row_info, segments, nodes)
    cable_after = mu + time_step * (cable_out + slope(u) * mu - drawn)
    mu_o[...] = cable_after
    inner = jnp.sum(differences * lane_differences(u), axis=1, keepdims=True)
    head = (mu[:, 0:1] - parent_tail) * (to_column(parent_old[...]) - u[:, 0:1])
    cable_grad = to_row(time_step * (jnp.where(info["parent"] >= 0.0, head, 0.0) - inner))
    grad_row_o[...] = grad_row[...] + cable_grad if last else cable_grad

    for each in started:
        each.wait()

    def finish(x, a, v, flux, product):
        after = a + time_step * (flux + slope(v) * a + sum_r[x])
        next_r[x] = after
        grad = (-0.5 * time_step) * product
        if last:
            g_r[x] = g_r[x] + grad
        else:
            g_r[x] = grad
            high, low = parts(after)
            high_r[pl.ds(x * cells_y, cells_y), :] = high
            low_r[pl.ds(x * cells_y, cells_y), :] = low

    v_first, s_edge = first_edges(first_edge, cells_x, cells_y)
    v_edge = v_first if last else (vup2, vdn2, vup1, vdn1, 0, 0)
    adjoint_steps(a_r, v_r, s_r, edge + (0, 0), v_edge, s_edge, side, finish)
    out_lam = copy(next_r, lam_h, sems.at[4])
    out_grad = copy(g_r, grad_h, sems.at[5])
    if not last:
        sent_o, out_up2, out_dn2, out_up1, out_dn1 = outs[4:]
        store_faces(next_r, out_up2, out_dn2, out_up1, out_dn1)
        sent_o[:, 0, 0:capacity] = tissue_gather(high_r, low_r, line_r, lane_r, value_r, devices)
        sent_o[:, 0, capacity:width] = slots_out(
            node_gather(cable_after, info), info, row_info, devices, capacity
        )
        for ref in (out_up2, out_dn2, out_up1, out_dn1):
            count = ref.shape[0]
            ref[count - 8 : count, :] = jnp.zeros((8, cells_z), f32)
        store_ends(cable_after, cells_y, cells_x, out_up2, out_dn2, out_up1, out_dn1)
    out_lam.wait()
    out_grad.wait()


def shifted(block, distance):
    axes = ("gx", "gy")
    devices = range(lax.axis_size(axes))
    return lax.ppermute(block, axes, [(i - distance, i) for i in devices if i - distance in devices])


def neighbours(up2, dn2, up1, dn1):
    moved = []
    for block, distance in ((up2, 2), (dn2, -2), (up1, 1), (dn1, -1)):
        moved.append(shifted(block, distance))
    return moved


def swap_slots(slots):
    return lax.all_to_all(slots, ("gx", "gy"), split_axis=0, concat_axis=0, tiled=True)


def body(
    initial_voltage,
    conductivity,
    tissue_mask,
    target_step,
    initial_purkinje,
    purkinje_conductivity,
    segment_parent,
    purkinje_target,
    junction_voxel,
    junction_node,
):
    shape = initial_voltage.shape
    cells_x, cells_y, cells_z = shape
    segments, nodes = initial_purkinje.shape
    grid_x, grid_y = lax.axis_size("gx"), lax.axis_size("gy")
    devices = grid_x * grid_y
    per_device = junction_voxel.shape[0]
    capacity = max(2, 2 * per_device // devices)
    slots = devices * capacity
    plane = cells_y * grid_y * cells_z
    side = lax.axis_index("gy")
    first = lax.axis_index(("gx", "gy")) * segments
    scal = jnp.stack([side, first]).astype(i32)
    one = sds((1, segments))
    cable_shape = sds((segments, nodes))
    tissue_shape = sds(shape)
    double = sds((devices, 1, 2 * capacity))
    faces = [sds((n, cells_z)) for n in (cells_y, cells_y, cells_x, cells_x)]
    payload = [sds((n + 8, cells_z)) for n in (cells_y, cells_y, cells_x, cells_x)]
    payload0 = [sds((2 * n + 8, cells_z)) for n in (cells_y, cells_y, cells_x, cells_x)]
    whole = pltpu.VMEM(shape, f32)
    whole_int = pltpu.VMEM(shape, i32)
    work = field_scratch(slots, shape)

    sent0, info, rows, *out0 = call(
        functools.partial(setup_kernel, plane, cells_y, cells_z, cells_x, grid_y),
        near(double, sds((segments, 128)), sds((8, segments)), *payload0),
        near(
            junction_voxel.reshape(1, -1),
            junction_node.reshape(1, -1),
            segment_parent.reshape(1, -1),
            purkinje_conductivity.reshape(1, -1),
            initial_purkinje,
        )
        + far(initial_voltage, conductivity, tissue_mask),
        [
            pltpu.VMEM((2, cells_y, cells_z), f32),
            pltpu.VMEM((2, cells_y, cells_z), f32),
            pltpu.VMEM((2, cells_y, cells_z), i32),
            pltpu.VMEM((2, cells_x, 8, cells_z), f32),
            pltpu.VMEM((2, cells_x, 8, cells_z), f32),
            pltpu.VMEM((2, cells_x, 8, cells_z), i32),
            DMA((12,)),
        ],
        scal,
    )
    arrived0 = swap_slots(sent0)
    edge0 = neighbours(*out0)
    own0 = out0[3]

    voltage1, soft, sent1, *faces1 = call(
        tissue_first_kernel,
        far(tissue_shape, tissue_shape) + near(double, *faces),
        near(arrived0, info, *edge0) + far(initial_voltage, conductivity, tissue_mask),
        work + [whole, whole, whole_int, whole, DMA((5,))],
    )
    arrived1 = swap_slots(sent1)
    cable1, sent2, there1, parent0, *out1 = call(
        cable_first_kernel,
        near(cable_shape, sds((devices, 1, capacity)), one, one, *payload),
        near(arrived1, initial_purkinje, info, rows, own0, *edge0, *faces1),
    )
    arrived2 = swap_slots(sent2)
    edge1 = neighbours(*out1)
    voltage2, lam2, cable2, mu2, sent3, parent1, *out2 = call(
        middle_kernel,
        far(tissue_shape, tissue_shape) + near(cable_shape, cable_shape, double, one, *payload),
        near(arrived2, sent1, arrived0, info, rows, own0, *edge0, *edge1, cable1, purkinje_target, there1)
        + far(voltage1, soft, target_step),
        work + [whole, whole, whole_int, whole, whole, DMA((5,))],
    )

    def backward(last, sent, out, lam, volt, volt_edge, mu, old, parent_old, grads):
        arrived = swap_slots(sent)
        edge = neighbours(*out)
        outs = far(tissue_shape, tissue_shape) + near(cable_shape, one)
        if not last:
            outs += near(double, *payload)
        return call(
            functools.partial(backward_kernel, last),
            outs,
            near(arrived, sent, arrived0, info, rows, own0, *edge0, *volt_edge, *edge)
            + near(mu, old, parent_old, grads[1])
            + far(lam, volt, soft, grads[0]),
            work + [whole, whole, whole, whole, whole, DMA((6,))],
        )

    lam1, grad, mu1, grad_row, sent4, *out3 = backward(
        False, sent3, out2, lam2, voltage1, edge1, mu2, cable1, parent1, (lam2, parent1)
    )
    lam0, grad, mu0, grad_row = backward(
        True, sent4, out3, lam1, initial_voltage, edge1, mu1, initial_purkinje, parent0, (grad, grad_row)
    )
    return (voltage2, cable2, grad, grad_row.reshape(-1), lam0, mu0)


def solution(mesh):
    tissue = P(("groups", "gx"), "gy", None)
    cable = P(("groups", "gx", "gy"), None)
    flat = P(("groups", "gx", "gy"))
    in_specs = (tissue, tissue, tissue, tissue, cable, flat, flat, cable, flat, flat)
    out_specs = (tissue, cable, tissue, flat, tissue, cable)
    return jax.shard_map(body, mesh=mesh, in_specs=in_specs, out_specs=out_specs, check_vma=False)
```
